32 devices in a mesh: rep: 2 (over z, core), dp: 16 (over x, y).
Axes of the slice: x: 4, y: 4, z: 1, core: 2. Of those that a mesh axis runs over, the one named last changes fastest.
The devices are a block of a 4x4x8 slice.
Arguments:
- x: bfloat16 [32, 2048, 512], P(('rep', 'dp')), parts along dimension 0
- dy: bfloat16 [32, 2048, 512], P(('rep', 'dp')), parts along dimension 0
- wq: bfloat16 [2, 512, 512], replicated
- wk: bfloat16 [2, 512, 512], replicated
- wv: bfloat16 [2, 512, 512], replicated
- wo: bfloat16 [2, 512, 512], replicated
- w_gate: bfloat16 [2, 512, 2048], replicated
- w_up: bfloat16 [2, 512, 2048], replicated
- w_down: bfloat16 [2, 2048, 512], replicated
- m_wq: float32 [2, 512, 512], replicated
- m_wk: float32 [2, 512, 512], replicated
- m_wv: float32 [2, 512, 512], replicated
- m_wo: float32 [2, 512, 512], replicated
- m_w_gate: float32 [2, 512, 2048], replicated
- m_w_up: float32 [2, 512, 2048], replicated
- m_w_down: float32 [2, 2048, 512], replicated
- v_wq: float32 [2, 512, 512], replicated
- v_wk: float32 [2, 512, 512], replicated
- v_wv: float32 [2, 512, 512], replicated
- v_wo: float32 [2, 512, 512], replicated
- v_w_gate: float32 [2, 512, 2048], replicated
- v_w_up: float32 [2, 512, 2048], replicated
- v_w_down: float32 [2, 2048, 512], replicated
Outputs:
- output 1: bfloat16 [4, 512, 512], P('rep'), parts along dimension 0
- output 2: bfloat16 [4, 512, 512], P('rep'), parts along dimension 0
- output 3: bfloat16 [4, 512, 512], P('rep'), parts along dimension 0
- output 4: bfloat16 [4, 512, 512], P('rep'), parts along dimension 0
- output 5: bfloat16 [4, 512, 2048], P('rep'), parts along dimension 0
- output 6: bfloat16 [4, 512, 2048], P('rep'), parts along dimension 0
- output 7: bfloat16 [4, 2048, 512], P('rep'), parts along dimension 0
- output 8: float32 [4, 512, 512], P('rep'), parts along dimension 0
- output 9: float32 [4, 512, 512], P('rep'), parts along dimension 0
- output 10: float32 [4, 512, 512], P('rep'), parts along dimension 0
- output 11: float32 [4, 512, 512], P('rep'), parts along dimension 0
- output 12: float32 [4, 512, 2048], P('rep'), parts along dimension 0
- output 13: float32 [4, 512, 2048], P('rep'), parts along dimension 0
- output 14: float32 [4, 2048, 512], P('rep'), parts along dimension 0
- output 15: float32 [4, 512, 512], P('rep'), parts along dimension 0
- output 16: float32 [4, 512, 512], P('rep'), parts along dimension 0
- output 17: float32 [4, 512, 512], P('rep'), parts along dimension 0
- output 18: float32 [4, 512, 512], P('rep'), parts along dimension 0
- output 19: float32 [4, 512, 2048], P('rep'), parts along dimension 0
- output 20: float32 [4, 512, 2048], P('rep'), parts along dimension 0
- output 21: float32 [4, 2048, 512], P('rep'), parts along dimension 0
There are 2 independent parts. The reference program is written for one: setup_inputs(seed, part) draws one part's arguments, and reference() takes and returns one part's arrays. A program takes and returns all parts, laid end to end along the dimension named above; an argument that names none is the same for every part.
All inputs are finite; a program needn't handle non-finite values.
Results may differ from the reference program's by a relative error of at most 0.024.
Values are sent between devices in bfloat16 or wider.
A program may use at most 768 MiB of HBM per device.

```python
import jax
import jax.numpy as jnp
from jax import lax

SEQUENCES = 16
TOKENS = 2048
D = 512
HEADS = 4
KV_HEADS = 4
HEAD = 128
FF = 2048
LAYERS = 2
THETA = 10000
NAMES = ("wq", "wk", "wv", "wo", "w_gate", "w_up", "w_down")
SHAPES = {
    "wq": (LAYERS, D, HEADS * HEAD),
    "wk": (LAYERS, D, KV_HEADS * HEAD),
    "wv": (LAYERS, D, KV_HEADS * HEAD),
    "wo": (LAYERS, HEADS * HEAD, D),
    "w_gate": (LAYERS, D, FF),
    "w_up": (LAYERS, D, FF),
    "w_down": (LAYERS, FF, D),
}


def bump(key, n, height):
    away = (jnp.arange(n, dtype=jnp.int32) - jax.random.randint(key, (), 0, n, jnp.int32)) % n
    return jnp.where(away < n // 8, height, 1.0)


def together(key, own, strength):
    shared = jax.random.normal(key, own.shape[1:], jnp.float32)
    return (own + strength * shared) * lax.rsqrt(1 + strength * strength)


def setup_inputs(seed: int = 0, part: int = 0) -> dict:
    kx, kdy, ka, kb, kz, kf, kh, kl, *keys = jax.random.split(jax.random.key(seed), 8 + 3 * len(NAMES))
    kx, kdy, ka, kb = (jax.random.fold_in(k, part) for k in (kx, kdy, ka, kb))
    kw, km, kv = (keys[i::3] for i in range(3))
    shape = (SEQUENCES, TOKENS, D)
    much_x, much_dy = jax.random.uniform(kz, (2,), jnp.float32, 0.0, 1.0)
    loud = 2.0 ** jax.random.uniform(jax.random.fold_in(kz, 1), (), jnp.float32, -1.0, 2.0)
    layers = 2.0 ** jax.random.uniform(kl, (LAYERS, 1, 1), jnp.float32, -1.0, 1.0)
    times = {"wq": 1.0, "wk": 1.0, "wv": 2.0, "wo": layers, "w_gate": 1.0, "w_up": bump(kh, FF, 4.0), "w_down": layers}
    x = together(ka, jax.random.normal(kx, shape, jnp.float32), much_x) * bump(kf, D, 4.0)
    dy = together(kb, jax.random.normal(kdy, shape, jnp.float32), much_dy)
    drawn = {"x": x.astype(jnp.bfloat16), "dy": (loud * dy * (SEQUENCES * TOKENS) ** -0.5).astype(jnp.bfloat16)}
    for key, name in zip(kw, NAMES, strict=True):
        drawn[name] = (jax.random.normal(key, SHAPES[name], jnp.float32) * SHAPES[name][1] ** -0.5 * times[name]).astype(jnp.bfloat16)
    for key, name in zip(km, NAMES, strict=True):
        drawn[f"m_{name}"] = 0.1 * jax.random.normal(key, SHAPES[name], jnp.float32)
    for key, name in zip(kv, NAMES, strict=True):
        drawn[f"v_{name}"] = jax.random.uniform(key, SHAPES[name], jnp.float32, 0.02, 0.06)
    return drawn


def matmul(a, w):
    return jnp.dot(a, w, preferred_element_type=jnp.float32).astype(jnp.bfloat16)


def normed(h):
    wide = h.astype(jnp.float32)
    scale = lax.rsqrt(jnp.mean(wide**2, -1, keepdims=True) + 1e-6)
    return (wide * scale).astype(jnp.bfloat16)


def turned(t, theta):
    half = t.shape[-1] // 2
    angle = jnp.arange(t.shape[0], dtype=jnp.float32)[:, None] * theta ** (-jnp.arange(half, dtype=jnp.float32) / half)
    cos, sin = jnp.cos(angle)[:, None], jnp.sin(angle)[:, None]
    a, b = t[..., :half].astype(jnp.float32), t[..., half:].astype(jnp.float32)
    return jnp.concatenate([a * cos - b * sin, b * cos + a * sin], -1).astype(jnp.bfloat16)


def seen_by(q, k, v):
    tokens, kv = q.shape[0], k.shape[1]
    q = q.reshape(tokens, kv, -1, q.shape[-1])
    scores = jnp.einsum("tgsd,ugd->gstu", q.astype(jnp.float32), k.astype(jnp.float32)) * q.shape[-1] ** -0.5
    place = jnp.arange(tokens)
    weights = jax.nn.softmax(jnp.where(place[:, None] >= place, scores, -jnp.inf), -1).astype(jnp.bfloat16)
    return jnp.einsum("gstu,ugd->tgsd", weights.astype(jnp.float32), v.astype(jnp.float32)).astype(jnp.bfloat16).reshape(tokens, -1)


def layer(h, w):
    a = normed(h)
    q, k = (turned(matmul(a, w[name]).reshape(h.shape[0], -1, HEAD), THETA) for name in ("wq", "wk"))
    h = h + matmul(seen_by(q, k, matmul(a, w["wv"]).reshape(h.shape[0], -1, HEAD)), w["wo"])
    b = normed(h)
    gate = jnp.dot(b, w["w_gate"], preferred_element_type=jnp.float32)
    up = jnp.dot(b, w["w_up"], preferred_element_type=jnp.float32)
    return h + matmul((jax.nn.silu(gate) * up).astype(jnp.bfloat16), w["w_down"])


def adamw(w, m, v, g):
    m = 0.9 * m + 0.1 * g
    v = 0.95 * v + 0.05 * g * g
    step = m * lax.rsqrt(v + 1e-8) + 0.1 * w
    return (w - 0.02 * step).astype(jnp.bfloat16), m, v


def clipped(gradients, sum_of_squares, count):
    factor = jnp.minimum(1.0, 0.5 * lax.rsqrt(sum_of_squares / count + 1e-30))
    return [g * factor for g in gradients]


def stack(weights, h):
    return lax.scan(lambda h, w: (layer(h, w), None), h, weights)[0]


def reference(x, dy, wq, wk, wv, wo, w_gate, w_up, w_down, m_wq, m_wk, m_wv, m_wo, m_w_gate, m_w_up, m_w_down, v_wq, v_wk, v_wv, v_wo, v_w_gate, v_w_up, v_w_down):
    weights = dict(zip(NAMES, (wq, wk, wv, wo, w_gate, w_up, w_down), strict=True))

    def take(so_far, sequence):
        h, by_y = sequence
        _, back = jax.vjp(stack, weights, h)
        by_weights, by_h = back(by_y)
        return jax.tree.map(lambda total, term: total + term.astype(jnp.float32), so_far, by_weights), by_h

    none_yet = {name: jnp.zeros(w.shape, jnp.float32) for name, w in weights.items()}
    by_weights, by_x = lax.scan(take, none_yet, (x, dy))
    gradients = [by_weights[name].astype(jnp.bfloat16).astype(jnp.float32) for name in NAMES]
    gradients = clipped(gradients, sum(jnp.sum(g * g) for g in gradients), sum(g.size for g in gradients))
    first = (m_wq, m_wk, m_wv, m_wo, m_w_gate, m_w_up, m_w_down)
    second = (v_wq, v_wk, v_wv, v_wo, v_w_gate, v_w_up, v_w_down)
    new = [adamw(weights[name].astype(jnp.float32), m, v, g) for name, m, v, g in zip(NAMES, first, second, gradients, strict=True)]
    return tuple(one[which] for which in range(3) for one in new)
```

```python
import argparse
import functools
import itertools

import jax
import jax.numpy as jnp
import numpy as np
from jax import lax
from jax.experimental import pallas as pl
from jax.experimental.pallas import tpu as pltpu
from jax.sharding import PartitionSpec as P

HEAD=128; THETA=10000
BF=jnp.bfloat16; F32=jnp.float32
VMEM = 56 * 2**20
LOG2E = 1.4426950408889634
HUGE = -1e30

def _dot(a, b, ca=1, cb=0):
    return lax.dot_general(a, b, (((ca,), (cb,)), ((), ())), preferred_element_type=F32)

def _dot_t(a, b):
    return _dot(a, b, 1, 1)

def _get(ref):
    return ref[...]

def _loop(many, what):
    lax.fori_loop(0, many, lambda i, _: what(i), None)

def _cut(refs, *sizes):
    refs = iter(refs)
    return [list(itertools.islice(refs, size)) for size in sizes] + [list(refs)]

def _params(*sem, limit=VMEM):
    return pltpu.CompilerParams(dimension_semantics=sem, vmem_limit_bytes=limit)

def turns(tokens, block):
    half = HEAD // 2
    speed = THETA ** (-np.arange(half) / half)
    def pair(places):
        angle = places[:, None] * speed
        return (np.concatenate([np.cos(angle)] * 2, 1).astype(np.float32), np.concatenate([np.sin(angle)] * 2, 1).astype(np.float32))
    return (*pair(np.arange(block)), *pair(np.arange(0, tokens, block)))

def _rms(h):
    wide = h.astype(F32)
    return wide, lax.rsqrt(jnp.mean(wide * wide, -1, keepdims=True) + 1e-6)

def _angles(i, cl, sl, ch, sh):
    c0, s0 = ch[pl.ds(i, 1), :], sh[pl.ds(i, 1), :]
    c = _get(cl) * c0 - _get(sl) * s0
    s = _get(sl) * c0 + _get(cl) * s0
    lane = lax.broadcasted_iota(jnp.int32, s.shape, 1)
    return c, jnp.where(lane < HEAD // 2, -s, s)

def _qkv(h_ref, wq, wk, wv, cl, sl, ch, sh, q_ref, k_ref, v_ref):
    i = pl.program_id(0)
    wide, scale = _rms(_get(h_ref))
    a = (wide * scale).astype(BF)
    c, s = _angles(i, cl, sl, ch, sh)
    for w, out in ((wq, q_ref), (wk, k_ref)):
        t = _dot(a, _get(w)).astype(BF).astype(F32)
        for n in range(0, t.shape[1], HEAD):
            one = t[:, n:n+HEAD]
            out[:, n:n+HEAD] = (one * c + pltpu.roll(one, HEAD//2, 1) * s).astype(BF)
    v_ref[...] = _dot(a, _get(wv)).astype(BF)

def _weight(w, layer):
    return pl.BlockSpec((None, *w.shape[1:]), lambda *_: (layer, 0, 0), pipeline_mode=pl.Buffered(1))

def qkv(h, wq, wk, wv, layer, block=512):
    t, d = h.shape
    tables = turns(t, block)
    rows = pl.BlockSpec((block, d), lambda i: (i, 0))
    whole = lambda a: pl.BlockSpec(a.shape, lambda i: (0, 0), pipeline_mode=pl.Buffered(1))
    outs = [w.shape[2] for w in (wq, wk, wv)]
    return pl.pallas_call(_qkv, grid=(t // block,),
        in_specs=[rows, *(_weight(w, layer) for w in (wq, wk, wv)), *(whole(a) for a in tables)],
        out_specs=[pl.BlockSpec((block, n), lambda i: (i, 0)) for n in outs],
        out_shape=[jax.ShapeDtypeStruct((t, n), BF) for n in outs],
        compiler_params=_params("arbitrary"),
        cost_estimate=pl.CostEstimate(flops=2*t*d*sum(outs), bytes_accessed=2*t*(d+sum(outs)), transcendentals=0),
        name="qkv")(h, wq, wk, wv, *(jnp.asarray(a) for a in tables))

def _ffn(o_ref, h_ref, wo, wg, wu, wd, out_ref, *, wide):
    h1 = (_get(h_ref).astype(F32) + _dot(_get(o_ref), _get(wo)).astype(BF).astype(F32)).astype(BF)
    x, scale = _rms(h1)
    b = (x * scale).astype(BF)
    total = None
    for c in range(0, wg.shape[1], wide):
        gate = _dot(b, wg[:, c:c+wide])
        up = _dot(b, wu[:, c:c+wide])
        act = (gate * lax.logistic(gate) * up).astype(BF)
        one = _dot(act, wd[c:c+wide, :])
        total = one if total is None else total + one
    out_ref[...] = (h1.astype(F32) + total.astype(BF).astype(F32)).astype(BF)

def ffn(o, h, wo, wg, wu, wd, layer, block=512, wide=512):
    t, d = h.shape
    rows = lambda n: pl.BlockSpec((block, n), lambda i: (i, 0))
    return pl.pallas_call(functools.partial(_ffn, wide=wide), grid=(t // block,),
        in_specs=[rows(o.shape[1]), rows(d), *(_weight(w, layer) for w in (wo, wg, wu, wd))],
        out_specs=rows(d), out_shape=jax.ShapeDtypeStruct((t, d), BF),
        compiler_params=_params("arbitrary"),
        cost_estimate=pl.CostEstimate(flops=2*t*(d*o.shape[1]+3*d*wg.shape[2]), bytes_accessed=6*t*d, transcendentals=0),
        name="ffn")(o, h, wo, wg, wu, wd)


def _attend_s(q_ref, k_ref, v_ref, o_ref, lse_ref, vt_s, top_s, mix_s, *, heads, bq, scale):
    iq = pl.program_id(0)
    e = scale * LOG2E
    half = bq // 2
    cols = [pl.ds(n * HEAD, HEAD) for n in range(heads)]
    cut = [pl.ds(n * (HEAD + 8), HEAD + 8) for n in range(heads)]
    mine = pl.ds(pl.multiple_of(iq * bq, bq), bq)
    for n, c in enumerate(cols):
        vt_s[n * (HEAD + 8):n * (HEAD + 8) + HEAD, mine] = v_ref[pl.ds(iq * bq, bq), c].T
        vt_s[n * (HEAD + 8) + HEAD:(n + 1) * (HEAD + 8), mine] = jnp.ones((8, bq), BF)
    top_s[...] = jnp.full_like(top_s, HUGE)
    mix_s[...] = jnp.zeros_like(mix_s)

    def block(at, size, pieces, ok):
        here, lane = pl.ds(at, size), pl.ds(pl.multiple_of(at, 128), size)
        scores = [_dot_t(k_ref[here, cols[n]], q_ref[a:a+w, cols[n]]) for n, a, w in pieces]
        ps, keeps = [], []
        for (n, a, w), s in zip(pieces, scores):
            if ok is not None:
                s = jnp.where(ok, s, 2 * HUGE)
            old = top_s[n:n+1, a:a+w]
            new = jnp.maximum(old, s.max(axis=0, keepdims=True))
            top_s[n:n+1, a:a+w] = new
            ps.append(jnp.exp2((s - new) * e).astype(BF))
            keeps.append(jnp.exp2((old - new) * e))
        for (n, a, w), p, keep in zip(pieces, ps, keeps):
            mix_s[cut[n], a:a+w] = mix_s[cut[n], a:a+w] * keep + _dot(vt_s[cut[n], lane], p)
    _loop(iq, lambda j: block(j * bq, bq, [(n, 0, bq) for n in range(heads)], None))
    seen = lambda w: lax.broadcasted_iota(jnp.int32, (half, w), 1) >= lax.broadcasted_iota(jnp.int32, (half, w), 0)
    block(iq * bq, half, [(n, 0, bq) for n in range(heads)], seen(bq))
    block(iq * bq + half, half, [(n, half, half) for n in range(heads)], seen(half))
    for n, c in enumerate(cols):
        total = mix_s[n * (HEAD + 8) + HEAD:n * (HEAD + 8) + HEAD + 1, :]
        o_ref[:, c] = (mix_s[n * (HEAD + 8):n * (HEAD + 8) + HEAD, :] * (1 / total)).T.astype(BF)
        lse_ref[n:n+1, :] = top_s[n:n+1, :] * e + jnp.log2(total)

def attend(q, k, v, bq=512):
    t, w = q.shape
    heads = w // HEAD
    rows = pl.BlockSpec((bq, w), lambda i: (i, 0))
    return pl.pallas_call(functools.partial(_attend_s, heads=heads, bq=bq, scale=HEAD**-0.5), grid=(t // bq,),
        in_specs=[rows, pl.BlockSpec((t, w), lambda i: (0, 0)), pl.BlockSpec((t, w), lambda i: (0, 0))],
        out_specs=[rows, pl.BlockSpec((heads, bq), lambda i: (0, i))],
        out_shape=[jax.ShapeDtypeStruct((t, w), BF), jax.ShapeDtypeStruct((heads, t), F32)],
        scratch_shapes=[pltpu.VMEM((heads * (HEAD + 8), t), BF), pltpu.VMEM((heads, bq), F32), pltpu.VMEM((heads * (HEAD + 8), bq), F32)],
        compiler_params=_params("arbitrary"),
        cost_estimate=pl.CostEstimate(flops=2*t*t*w, bytes_accessed=8*t*w, transcendentals=heads*t*t//2), name="attend")(q, k, v)


MESH = pl.DeviceIdType.MESH

class Ring:
    def __init__(self, side):
        self.side, self.me = side, lax.axis_index("dp")
        at = self.me // side, self.me % side
        self.places = [[lax.rem(place + k, side) for k in range(side)] for place in at]

    def place(self, axis, away=0):
        return self.places[axis][away % self.side]

    def next(self, axis, sign):
        x, y = (self.place(n, sign if n == axis else 0) for n in range(2))
        return x * self.side + y

    def greet(self, far):
        many = self.side**2
        peers = [lax.rem(self.me + k, many) for k in range(1, many)] if far else [self.next(c // 2, _sign(c)) for c in range(4)]
        for peer in peers:
            pl.semaphore_signal(pltpu.get_barrier_semaphore(), inc=1, device_id={"dp": peer}, device_id_type=MESH)
        return peers


def _sign(c):
    return 1 - c % 2 * 2


def _each(what, many=4):
    for c in range(many):
        what(c)


def _send(src, dst, send, recv, to):
    return pltpu.make_async_remote_copy(src_ref=src, dst_ref=dst, send_sem=send, recv_sem=recv, device_id={"dp": to}, device_id_type=MESH)


def _rows(ref, at, size):
    return ref.at[:, pl.ds(pl.multiple_of(at, size), size), :]


class Scatter:
    steps, parts = 4, 5

    def __init__(self, ring, own, buffers, send, recv, result):
        self.ring, self.own, self.send, self.recv, self.result = ring, own, send, recv, result
        self.xa, self.xb, self.ya_out, self.ya, self.yb_out, self.yb = buffers
        self.big, self.small = self.xb.shape[-2], self.yb.shape[-2]

    def mine(self, c, part, rows, size):
        return _rows(self.own.at[c // 2], self.ring.place(c // 2, part) * self.big + rows, size)

    def copies(self, c, s):
        sign, axis = _sign(c), (c // 2 + s // 2) % 2
        half = self.big // 2
        rows, other = c % 2 * half, (1 - c % 2) * half
        if s == 0:
            pairs = [(self.mine(c, 2, rows, half), self.xa.at[c])]
        elif s == 1:
            pairs = [(self.xa.at[c], _rows(self.xb.at[c], rows, half)), (self.mine(c, sign, other, half), _rows(self.xb.at[c], other, half))]
        else:
            pairs = [(self.ya_out.at[c], self.ya.at[c]) if s == 2 else (self.yb_out.at[c], self.yb.at[c])]
        return [_send(a, b, self.send.at[c, s + s // 2 + n], self.recv.at[c, s + s // 2 + n], self.ring.next(axis, sign)) for n, (a, b) in enumerate(pairs)]

    def total(self, half, part, rows, size):
        at = self.ring.place(1 - half, part) * self.small + rows
        got = [_get(_rows(self.xb.at[2 * half + n], at, size)).astype(F32) for n in range(2)]
        return got[0] + got[1] + _get(self.mine(2 * half, 0, at, size)).astype(F32)

    def ready(self, c, s):
        sign, half = _sign(c), self.small // 2
        rows = c % 2 * half
        if s == 1:
            self.xa[c] = (self.xa[c].astype(F32) + _get(self.mine(c, sign, c % 2 * (self.big // 2), self.big // 2)).astype(F32)).astype(BF)
        elif s == 2:
            self.ya_out[c] = self.total(c // 2, 2, rows, half).astype(BF)
        elif s == 3:
            _rows(self.yb_out.at[c], half - rows, half)[...] = self.total(c // 2, sign, half - rows, half).astype(BF)
            _rows(self.yb_out.at[c], rows, half)[...] = (self.total(c // 2, sign, rows, half) + self.ya[c].astype(F32)).astype(BF)

    def step(self, s):
        if s:
            _each(lambda c: [one.wait_recv() for one in self.copies(c, s - 1)])
        if s == self.steps:
            def close(half):
                total = self.total(half, 0, 0, self.small)
                self.result(half)[...] = (total + self.yb[2 * half].astype(F32) + self.yb[2 * half + 1].astype(F32)).astype(BF)
            _each(close, 2)
            return
        if s:
            _each(lambda c: self.ready(c, s))
        _each(lambda c: [one.start() for one in self.copies(c, s)])


class Gather:
    steps, parts = 4, 4

    def __init__(self, ring, whole, send, recv, base):
        self.ring, self.whole, self.send, self.recv, self.base = ring, whole, send, recv, base
        self.big = whole.shape[-2] // ring.side

    def place(self, half):
        small = self.big // self.ring.side
        return _rows(self.whole.at[half], self.ring.place(half) * self.big + self.ring.place(1 - half) * small, small)

    def copies(self, c, s):
        ring, sign, half = self.ring, _sign(c), c // 2
        axis = (1 - half) if s < 2 else half
        size = self.big // ring.side if s < 2 else self.big
        far = s % 2
        at = ring.place(axis, -sign * far) * size + far * (c % 2) * (size // 2)
        if s < 2:
            at = ring.place(half) * self.big + at
        part = _rows(self.whole.at[half], at, size // (1 + far))
        return [_send(part, part, self.send.at[c, self.base + s], self.recv.at[c, self.base + s], ring.next(axis, sign))]

    def step(self, s):
        if s:
            _each(lambda c: self.copies(c, s - 1)[0].wait_recv())
        if s < self.steps:
            _each(lambda c: self.copies(c, s)[0].start())


class Job:
    def __init__(self, kind, matrices, time=1.0, made=False):
        self.kind, self.matrices, self.time, self.made = kind, matrices, time, made
        self.sums, self.shares = kind != "share", kind != "sum"

    def sizes(self):
        return [self.matrices * BIG * k for k in ([0.5, 1, 0.125, 0.25] * self.sums + [0.25, 0.125, 1, 0.5] * self.shares)]


BIG, LAG = 1.43, 2.5


def plan(jobs, times):
    wire, state, out = 0.0, [(0, job.time) for job in jobs], []
    now = 0.0
    def advance():
        nonlocal wire
        picks = []
        for j, job in enumerate(jobs):
            s, ready = state[j]
            sizes = job.sizes()
            if s <= len(sizes) and ready <= now:
                picks.append((j, s))
                if s < len(sizes):
                    wire = max(wire, now) + sizes[s]
                state[j] = (s + 1, wire + LAG)
        return picks
    for now in times:
        out.append(advance())
    rest = []
    while todo := [ready for (s, ready), job in zip(state, jobs) if s <= len(job.sizes())]:
        now = max(now, min(todo))
        rest += advance()
    return out + [rest]


class Traffic:
    def __init__(self, jobs, side, rows, times, far=False):
        self.jobs, self.side, self.rows, self.far = jobs, side, rows, far
        self.plan = plan(jobs, times)
        small = rows // side**2
        hbm, vmem = pl.BlockSpec(memory_space=pltpu.HBM), lambda *s: pl.BlockSpec(s, lambda *_: (0,) * len(s), pipeline_mode=pl.Buffered(1))
        self.in_specs, self.out_specs, self.out_shape, self.scratch = [], [], [], []
        for job in jobs:
            unit = lambda many, size: (many, job.matrices, size, rows // 2)
            if not job.made:
                self.in_specs.append(hbm if job.sums else vmem(*unit(2, small)))
            shape = unit(2, rows if job.shares else small)
            self.out_specs.append(hbm if job.shares else vmem(*shape))
            self.out_shape.append(jax.ShapeDtypeStruct(shape, BF))
            if job.sums:
                sizes = (rows // side // 2, rows // side, small // 2, small // 2, small, small)
                self.scratch += [pltpu.VMEM(unit(2, rows), BF)] * (not job.made) + [pltpu.VMEM(unit(4, size), BF) for size in sizes]
            if job.shares:
                self.scratch.append(pltpu.VMEM(unit(2, rows), BF))
            parts = Scatter.parts * job.sums + Gather.parts * job.shares
            self.scratch += [pltpu.SemaphoreType.DMA((4, parts))] * 2 + [pltpu.SemaphoreType.DMA((2,))]
        self.out_specs.append(vmem(8, HEAD))
        self.out_shape.append(jax.ShapeDtypeStruct((8, HEAD), F32))

    def bind(self, ins, outs, scratch, made=()):
        ins, outs, scratch, made = iter(ins), iter(outs), iter(scratch), iter(made)
        self.ring = Ring(self.side)
        self.run, self.mine = [], []
        for job in self.jobs:
            r = argparse.Namespace(given=None if job.made else next(ins), out=next(outs))
            if job.sums:
                r.own = next(made) if job.made else next(scratch)
                buffers = [next(scratch) for _ in range(6)]
            if job.shares:
                r.whole = next(scratch)
            send, recv, sem = (next(scratch) for _ in range(3))
            if job.shares:
                r.gather = Gather(self.ring, r.whole, send, recv, Scatter.parts * job.sums)
                r.store = pltpu.make_async_copy(r.whole, r.out, sem.at[1])
            if job.sums:
                r.scatter = Scatter(self.ring, r.own, buffers, send, recv, r.gather.place if job.shares else lambda half, r=r: r.out.at[half])
                r.load = None if job.made else pltpu.make_async_copy(r.given, r.own, sem.at[0])
            self.run.append(r)
        self.squares = next(outs)

    def start(self):
        for job, r in zip(self.jobs, self.run):
            if job.sums and not job.made:
                r.load.start()
        self.squares[...] = jnp.zeros_like(self.squares)
        self.peers = self.ring.greet(self.far)

    def meet(self):
        pl.semaphore_wait(pltpu.get_barrier_semaphore(), len(self.peers))

    def take(self, j, s):
        job, r = self.jobs[j], self.run[j]
        steps = Scatter.steps
        if s == 0 and not job.made and job.sums:
            r.load.wait()
        if job.sums and s <= steps:
            r.scatter.step(s)
            if s == steps:
                def fold(c):
                    got = r.scatter.result(c)[...].astype(F32)
                    got = (got * got).reshape(-1, 8, got.shape[-1]).sum(0)
                    self.squares[...] += sum(got[:, n:n + HEAD] for n in range(0, got.shape[-1], HEAD))
                _each(fold, 2)
        if job.shares and s >= steps * job.sums:
            if not job.sums and s == 0:
                def put(c):
                    r.gather.place(c)[...] = r.given[c]
                _each(put, 2)
            r.gather.step(s - steps * job.sums)
            if s == steps * (1 + job.sums):
                r.store.start()

    def tick(self, now, possible):
        for n in possible:
            picks = self.plan[n]
            if picks:
                @pl.when(now == n)
                def _():
                    for j, s in picks:
                        self.take(j, s)

    def finish(self):
        for j, s in self.plan[-1]:
            self.take(j, s)
        for job, r in zip(self.jobs, self.run):
            for part in ([r.scatter] if job.sums else []) + ([r.gather] if job.shares else []):
                for s in range(part.steps):
                    _each(lambda c: [one.wait_send() for one in part.copies(c, s)])
            if job.shares:
                r.store.wait()


def _once(*shape):
    return pl.BlockSpec(shape, lambda *_: (0,) * len(shape), pipeline_mode=pl.Buffered(1))

def _comm(ident):
    return pltpu.CompilerParams(dimension_semantics=("arbitrary",), vmem_limit_bytes=MOST, collective_id=ident, has_side_effects=True)

MOST = 63 * 2**20

def _norm_back(x, s, by):
    by = by.astype(BF).astype(F32)
    return (s * by - x * (s * s * s * jnp.mean(by * x, -1, keepdims=True))).astype(BF).astype(F32)


def _split(to, value):
    for half, part in enumerate(jnp.split(value, 2, 1)):
        to(half)[...] = part.astype(BF)

def _half(*refs, block, sub, traffic, n_in, n_out, n_rest):
    main, ins, rest, mine, outs, own, scratch = _cut(refs, 7, n_in, n_rest, 3, n_out, 10)
    o_ref, h_ref, dy_ref, wo, wg, wu, wd = main
    do_ref, delta_ref, dh_ref = mine
    h1_s, b_s, bt_s, dyt_s, act_s, dg_s, du_s, db_s, own_s, own_sem = own
    c, last = pl.program_id(0), own_s.shape[0] - 1
    t, d = h_ref.shape
    per = t // block
    units = [own_s.at[n, :, pl.ds(0, 3)] for n in range(last)] + [own_s.at[last]]
    traffic.bind(ins, outs, scratch, units[:len(units) - n_rest])
    keep = [pltpu.make_async_copy(a, b, own_sem.at[n]) for n, (a, b) in enumerate(zip(units[len(units) - n_rest:], rest))]
    at = lambda i: pl.ds(pl.multiple_of(i * block, block), block)

    @pl.when(c == 0)
    def _():
        traffic.start()
        def head(i):
            h1 = (h_ref[at(i), :].astype(F32) + _dot(o_ref[at(i), :], _get(wo)).astype(BF).astype(F32)).astype(BF)
            h1_s[at(i), :] = h1
            x, scale = _rms(h1)
            b = (x * scale).astype(BF)
            b_s[at(i), :] = b
            bt_s[:, at(i)] = b.T
            dyt_s[:, at(i)] = dy_ref[at(i), :].T
            db_s[at(i), :] = jnp.zeros((block, d), F32)
        _loop(per, head)
        traffic.meet()

    def body(i):
        traffic.tick(c * (per + 3) + i, [n for n in range((last + 1) * (per + 3)) if n % (per + 3) < per])
        rows = [pl.ds(i * block + k, sub) for k in range(0, block, sub)]
        first = [(_dot(b_s[r, :], _get(wg)), _dot(b_s[r, :], _get(wu)), _dot_t(dy_ref[r, :], _get(wd))) for r in rows]
        for r, (gate, up, dact) in zip(rows, first):
            dact = dact.astype(BF).astype(F32)
            sig = lax.logistic(gate)
            silu = gate * sig
            act_s[r, :] = (silu * up).astype(BF)
            du = (dact * silu).astype(BF)
            dg = (dact * up * (sig + silu * (1 - sig))).astype(BF)
            du_s[r, :] = du
            dg_s[r, :] = dg
            db_s[r, :] += _dot_t(dg, _get(wg)) + _dot_t(du, _get(wu))
    _loop(per, body)
    for m, value in enumerate((lambda: _dot(_get(bt_s), _get(dg_s)), lambda: _dot(_get(bt_s), _get(du_s)), lambda: _dot(_get(dyt_s), _get(act_s)).T)):
        traffic.tick(c * (per + 3) + per + m, range(per + m, (last + 1) * (per + 3), per + 3))
        _split(lambda k: own_s.at[c, k, m], value())

    @pl.when(c == last)
    def _():
        def tail(i):
            traffic.tick((last + 1) * (per + 3) + i, range((last + 1) * (per + 3), len(traffic.plan) - 1))
            x, s = _rms(h1_s[at(i), :])
            dh = (dy_ref[at(i), :].astype(F32) + _norm_back(x, s, db_s[at(i), :])).astype(BF)
            dh_ref[at(i), :] = dh
            do = _dot_t(dh, _get(wo)).astype(BF)
            do_ref[at(i), :] = do
            prod = do.astype(F32) * o_ref[at(i), :].astype(F32)
            lane = lax.broadcasted_iota(jnp.int32, (block, HEAD), 1)
            sums = jnp.zeros((block, HEAD), F32)
            for n in range(prod.shape[1] // HEAD):
                sums = jnp.where(lane == n, prod[:, n*HEAD:(n+1)*HEAD].sum(-1, keepdims=True), sums)
            delta_ref[:, at(i)] = sums.T[:delta_ref.shape[0], :]
        _loop(per, tail)
        _split(lambda k: own_s.at[last, k, 3], _dot(_get(o_ref), _get(dh_ref), 0, 0))
        for one in keep:
            one.start()
        traffic.finish()
        for one in keep:
            one.wait()

def half_back(o, h, dy, wo, wg, wu, wd, layer, early, jobs, given, side, ident, block=512, sub=256, start=5.5, pace=1.75, dots=1.15, slow=1.3):
    t, d = h.shape
    e, f = o.shape[1], wg.shape[2]
    chunks, per = f // d, t // block
    times = []
    for c in range(chunks):
        now = start + c * (pace * per + dots * 3)
        times += [now + pace * i for i in range(per)] + [now + pace * per + dots * i for i in range(3)]
    times += [start + chunks * (pace * per + dots * 3) + slow * i for i in range(per)]
    made = [Job("sum", 3, start + (c + 1) * (pace * per + dots * 3), True) for c in range(early)]
    rest = [3] * (chunks - early - 1) + [4]
    traffic = Traffic(made + jobs, side, d, times)
    col, row = pl.BlockSpec((None, d, d), lambda c: (layer, 0, c)), pl.BlockSpec((None, d, d), lambda c: (layer, c, 0))
    big = lambda kind: pltpu.VMEM((t, d), kind)
    return pl.pallas_call(functools.partial(_half, block=block, sub=sub, traffic=traffic, n_in=len(given), n_out=len(traffic.out_specs), n_rest=len(rest)), grid=(chunks,),
        in_specs=[_once(t, e), _once(t, d), _once(t, d), _weight(wo, layer), col, col, row, *traffic.in_specs],
        out_specs=[pl.BlockSpec(memory_space=pltpu.HBM)] * len(rest) + [_once(t, e), _once(e // HEAD, t), _once(t, d), *traffic.out_specs],
        out_shape=[jax.ShapeDtypeStruct((2, n, d, d // 2), BF) for n in rest] + [jax.ShapeDtypeStruct((t, e), BF), jax.ShapeDtypeStruct((e // HEAD, t), F32),
                   jax.ShapeDtypeStruct((t, d), BF), *traffic.out_shape],
        scratch_shapes=[big(BF), big(BF), pltpu.VMEM((d, t), BF), pltpu.VMEM((d, t), BF), big(BF), big(BF), big(BF), big(F32),
                        pltpu.VMEM((chunks, 2, 4, d, d // 2), BF), pltpu.SemaphoreType.DMA((chunks,)), *traffic.scratch],
        compiler_params=_comm(ident),
        cost_estimate=pl.CostEstimate(flops=2*t*(3*d*e+8*d*f), bytes_accessed=12*t*d, transcendentals=0),
        name="half_back")(o, h, dy, wo, wg, wu, wd, *given)

def _first(*refs, heads, bq, scale, deep, traffic, n_in, n_out):
    main, ins, (unit_ref,), dx_ref, outs, own, scratch = _cut(refs, 15, n_in, 1, deep, n_out, 8)
    q_ref, k_ref, v_ref, do_ref, lse_ref, delta_ref, h_ref, dh_ref, wq, wk, wv, cl, sl, ch, sh = main
    kt_s, dq_s, dk_s, dv_s, q_s, at_s, k_s, v_s = own
    iq, last = pl.program_id(0), h_ref.shape[0] // bq - 1
    e = scale * LOG2E
    half = bq // 2
    cols = [pl.ds(n * HEAD, HEAD) for n in range(heads)]
    at = lambda i: pl.ds(pl.multiple_of(i * bq, bq), bq)
    mine = at(iq)
    traffic.bind(ins, outs, scratch)

    @pl.when(iq == 0)
    def _():
        traffic.start()
    x, s = _rms(h_ref[mine, :])
    at_s[:, mine] = (x * s).astype(BF).T
    for c in cols:
        kt_s[c, mine] = k_ref[mine, c].T
    dq_s[...] = jnp.zeros_like(dq_s)
    dk_s[mine, :] = jnp.zeros((bq, k_ref.shape[1]), F32)
    dv_s[mine, :] = jnp.zeros((bq, k_ref.shape[1]), F32)

    def block(at, size, pieces, ok):
        here, lane = pl.ds(at, size), pl.ds(pl.multiple_of(at, HEAD), size)
        scores = [_dot_t(k_ref[here, cols[n]], q_ref[a:a+w, cols[n]]) for n, a, w in pieces]
        dps = [_dot_t(v_ref[here, cols[n]], do_ref[a:a+w, cols[n]]) for n, a, w in pieces]
        for (n, a, w), s, dp in zip(pieces, scores, dps):
            p = jnp.exp2(s * e - lse_ref[n:n+1, a:a+w])
            if ok is not None:
                p = jnp.where(ok, p, 0.0)
            ds = (p * (dp - delta_ref[n:n+1, a:a+w])).astype(BF)
            dv_s[here, cols[n]] += _dot(p.astype(BF), do_ref[a:a+w, cols[n]])
            dk_s[here, cols[n]] += _dot(ds, q_ref[a:a+w, cols[n]])
            dq_s[cols[n], a:a+w] += _dot(kt_s[cols[n], lane], ds)

    pl.when(iq == 0)(traffic.meet)
    before = iq * (iq + 1) // 2
    cuts = list(itertools.accumulate(range(1, last + 2), initial=0))
    *cuts, ticks = [n for n in cuts[:-1]] + [cuts[-1]]
    cuts = [n + k for k, n in enumerate(cuts)]
    def off(j):
        traffic.tick(before + j, [n for n in range(ticks) if n not in cuts])
        block(j * bq, bq, [(n, 0, bq) for n in range(heads)], None)
    _loop(iq, off)
    traffic.tick(before + iq, cuts)
    seen = lambda w: lax.broadcasted_iota(jnp.int32, (half, w), 1) >= lax.broadcasted_iota(jnp.int32, (half, w), 0)
    block(iq * bq, half, [(n, 0, bq) for n in range(heads)], seen(bq))
    block(iq * bq + half, half, [(n, half, half) for n in range(heads)], seen(half))

    def unturned(i, value):
        c, s = _angles(i, cl, sl, ch, sh)
        one = (value * scale).astype(BF).astype(F32)
        return (one * c - pltpu.roll(one, HEAD // 2, 1) * s).astype(BF)
    for c in cols:
        q_s[mine, c] = unturned(iq, dq_s[c, :].T)

    @pl.when(iq == last)
    def _():
        def tail(i):
            traffic.tick(ticks + i, range(ticks, ticks + last + 1))
            for c in cols:
                k_s[at(i), c] = unturned(i, dk_s[at(i), c])
            v_s[at(i), :] = dv_s[at(i), :].astype(BF)
            if deep:
                by = _dot_t(q_s[at(i), :], _get(wq)) + _dot_t(k_s[at(i), :], _get(wk)) + _dot_t(v_s[at(i), :], _get(wv))
                x, s = _rms(h_ref[at(i), :])
                dx_ref[0][at(i), :] = (dh_ref[at(i), :].astype(F32) + _norm_back(x, s, by)).astype(BF)
        _loop(last + 1, tail)
        for m, value in enumerate((q_s, k_s, v_s)):
            traffic.tick(ticks + last + 1 + m, [ticks + last + 1 + m])
            _split(lambda k: unit_ref.at[k, m], _dot(_get(at_s), _get(value)))
        traffic.finish()


def first_back(q, k, v, do, lse, delta, h, dh, wq, wk, wv, layer, deep, jobs, given, side, ident, bq=512, start=2.0, pace=3.5, more=3.2, end=1.3):
    t, w = q.shape
    d, heads = h.shape[1], w // HEAD
    now, times = start, []
    for i in range(t // bq):
        times += [now + pace * j for j in range(i + 1)]
        now += pace * i + more
    times += [now + end * i for i in range(t // bq + 3)]
    traffic = Traffic(jobs, side, d, times)
    rows, stats = pl.BlockSpec((bq, w), lambda i: (i, 0)), pl.BlockSpec((heads, bq), lambda i: (0, i))
    tables = [jnp.asarray(a) for a in turns(t, bq)]
    big = lambda kind: pltpu.VMEM((t, w), kind)
    return pl.pallas_call(functools.partial(_first, heads=heads, bq=bq, scale=HEAD**-0.5, deep=deep, traffic=traffic, n_in=len(given), n_out=len(traffic.out_specs)),
        grid=(t // bq,),
        in_specs=[rows, _once(t, w), _once(t, w), rows, stats, stats, _once(t, d), _once(t, d), *(_weight(m, layer) for m in (wq, wk, wv)),
                  *(_once(*a.shape) for a in tables), *traffic.in_specs],
        out_specs=[_once(2, 3, d, d // 2)] + [_once(t, d)] * deep + traffic.out_specs,
        out_shape=[jax.ShapeDtypeStruct((2, 3, d, d // 2), BF)] + [jax.ShapeDtypeStruct((t, d), BF)] * deep + traffic.out_shape,
        scratch_shapes=[pltpu.VMEM((w, t), BF), pltpu.VMEM((w, bq), F32), big(F32), big(F32), big(BF), pltpu.VMEM((d, t), BF), big(BF), big(BF), *traffic.scratch],
        compiler_params=_comm(ident),
        cost_estimate=pl.CostEstimate(flops=5*t*t*w, bytes_accessed=14*t*w, transcendentals=heads*t*t//2),
        name="first_back")(q, k, v, do, lse, delta, h, dh, wq, wk, wv, *tables, *given)

def _last(*refs, traffic, n_in, n_out, known, count):
    ins, known, (factor_ref,), outs, (sums_s, one_s, send, recv), scratch = _cut(refs, n_in, known, 1, n_out, 4)
    traffic.bind(ins, outs, scratch)
    traffic.start()
    traffic.meet()
    me, n = traffic.ring.me, traffic.side**2
    copy = lambda peer, slot: _send(one_s, sums_s.at[slot], send.at[lax.rem(peer - me + n, n)], recv.at[slot], peer)
    waiting = sum(job.sums for job in traffic.jobs)
    for j, s in traffic.plan[-1]:
        traffic.take(j, s)
        if traffic.jobs[j].sums and s == Scatter.steps:
            waiting -= 1
            if not waiting:
                one_s[...] = sum((_get(ref) for ref in known), _get(traffic.squares))
                sums_s[me] = _get(one_s)
                for peer in traffic.peers:
                    copy(peer, me).start()
    traffic.plan[-1].clear()
    for peer in traffic.peers:
        copy(peer, peer).wait_recv()
    total = sums_s[0]
    for k in range(1, n):
        total = total + sums_s[k]
    factor_ref[...] = jnp.broadcast_to(jnp.minimum(1.0, 0.5 * lax.rsqrt(jnp.sum(total, keepdims=True) / count + 1e-30)), factor_ref.shape)
    for peer in traffic.peers:
        copy(peer, me).wait_send()
    traffic.finish()

def last(jobs, given, known, count, rows, side, ident):
    traffic = Traffic(jobs, side, rows, [], True)
    tile = jax.ShapeDtypeStruct((8, HEAD), F32)
    n = side**2
    return pl.pallas_call(functools.partial(_last, traffic=traffic, n_in=len(given), n_out=len(traffic.out_specs), known=len(known), count=count), grid=(1,),
        in_specs=traffic.in_specs + [_once(*tile.shape)] * len(known), out_specs=[_once(*tile.shape)] + traffic.out_specs, out_shape=[tile] + traffic.out_shape,
        scratch_shapes=[pltpu.VMEM((n, *tile.shape), F32), pltpu.VMEM(tile.shape, F32), *[pltpu.SemaphoreType.DMA((n,))] * 2, *traffic.scratch],
        compiler_params=_comm(ident), name="last")(*given, *known)

def _adam(*refs, arrays, units, places, slots, ahead, piece):
    (factor_ref,), w, m, v, g, new, (w_s, m_s, v_s, g_s, load, store) = _cut(refs, 1, *[arrays] * 3, units, 3 * arrays)
    factor = factor_ref[:1, :1]
    d = w_s.shape[2]

    def loads(i):
        array, layer, row, col, unit, matrix, part = places[i]
        k = i % slots
        spot = lambda a: a.at[layer, pl.ds(row, piece), pl.ds(col, d)]
        pairs = [(spot(a[array]), b.at[k]) for a, b in ((w, w_s), (m, m_s), (v, v_s))] + [(g[unit].at[:, matrix, pl.ds(part, piece), :], g_s.at[k])]
        return [pltpu.make_async_copy(a, b, load.at[k, n]) for n, (a, b) in enumerate(pairs)]

    def stores(i):
        array, layer, row, col, *_ = places[i]
        k = i % slots
        return [pltpu.make_async_copy(a.at[k], new[n * arrays + array].at[layer, pl.ds(row, piece), pl.ds(col, d)], store.at[k, n])
                for n, a in enumerate((w_s, m_s, v_s))]

    def each(copies, what):
        for one in copies:
            getattr(one, what)()

    for i in range(min(ahead, len(places))):
        each(loads(i), "start")
    for i in range(len(places)):
        each(loads(i), "wait")
        k = i % slots
        def update(r):
            rows = pl.ds(r * 32, 32)
            for c in range(2):
                cols = pl.ds(c * (d // 2), d // 2)
                grad = g_s[k, c, rows, :].astype(F32) * factor
                first = 0.9 * m_s[k, rows, cols] + 0.1 * grad
                second = 0.95 * v_s[k, rows, cols] + 0.05 * grad * grad
                old = w_s[k, rows, cols].astype(F32)
                m_s[k, rows, cols] = first
                v_s[k, rows, cols] = second
                w_s[k, rows, cols] = (old - 0.02 * (first * lax.rsqrt(second + 1e-8) + 0.1 * old)).astype(BF)
        _loop(piece // 32, update)
        each(stores(i), "start")
        if i + ahead < len(places):
            if i + ahead >= slots:
                each(stores(i + ahead - slots), "wait")
            each(loads(i + ahead), "start")
    for i in range(max(len(places) - slots, 0), len(places)):
        each(stores(i), "wait")

def adam(factor, w, m, v, units, slots=16, ahead=10, piece=256):
    d = w[0].shape[1]
    places, flat = [], []
    for layer, mine in reversed(list(enumerate(units))):
        blocks = []
        for n in range(len(mine) - 1):
            blocks += [(4, 0, n * d, n, 0), (5, 0, n * d, n, 1), (6, n * d, 0, n, 2)]
        blocks += [(3, 0, 0, len(mine) - 2, 3)] + [(i, 0, 0, len(mine) - 1, i) for i in range(3)]
        places += [(array, layer, row + part, col, len(flat) + unit, matrix, part) for array, row, col, unit, matrix in blocks for part in range(0, d, piece)]
        flat += mine
    hbm = pl.BlockSpec(memory_space=pltpu.HBM)
    size = sum(a.size for a in w)
    return pl.pallas_call(functools.partial(_adam, arrays=len(w), units=len(flat), places=places, slots=slots, ahead=ahead, piece=piece), grid=(1,),
        in_specs=[_once(8, HEAD)] + [hbm] * (3 * len(w) + len(flat)), out_specs=[hbm] * (3 * len(w)),
        out_shape=[jax.ShapeDtypeStruct(a.shape, a.dtype) for a in (*w, *m, *v)],
        scratch_shapes=[pltpu.VMEM((slots, piece, d), BF), pltpu.VMEM((slots, piece, d), F32), pltpu.VMEM((slots, piece, d), F32), pltpu.VMEM((slots, 2, piece, d // 2), BF),
                        pltpu.SemaphoreType.DMA((slots, 4)), pltpu.SemaphoreType.DMA((slots, 3))],
        compiler_params=pltpu.CompilerParams(dimension_semantics=("arbitrary",), vmem_limit_bytes=VMEM),
        cost_estimate=pl.CostEstimate(flops=16*size, bytes_accessed=22*size, transcendentals=size), name="adam")(factor, *w, *m, *v, *flat)


def solution(mesh):
    side = round(mesh.shape["dp"] ** 0.5)

    def step(x, dy, *arrays):
        weights, m, v = (arrays[i : i + 7] for i in (0, 7, 14))
        wq, wk, wv, wo, wg, wu, wd = weights
        h0 = x[0]
        q0, k0, v0 = qkv(h0, wq, wk, wv, 0)
        o0, lse0 = attend(q0, k0, v0)
        h1 = ffn(o0, h0, wo, wg, wu, wd, 0)
        q1, k1, v1 = qkv(h1, wq, wk, wv, 1)
        o1, lse1 = attend(q1, k1, v1)
        add, share = (lambda n, kind=kind: Job(kind, n) for kind in ("sum", "share"))
        c12, c13, do1, delta1, by1, s10, s11, sq0 = half_back(o1, h1, dy[0], wo, wg, wu, wd, 1, 2, [], [], side, 0)
        attn1, by0, s12, s13, g10, g11, sq1 = first_back(q1, k1, v1, do1, lse1, delta1, h1, by1, wq, wk, wv, 1, True,
                                                         [add(3), add(4), share(3), share(3)], [c12, c13, s10, s11], side, 1)
        c02, c03, do0, delta0, by, s00, s01, s14, g12, g13, sq2 = half_back(o0, h0, by0, wo, wg, wu, wd, 0, 2, [add(3), share(3), share(4)], [attn1, s12, s13], side, 2)
        attn0, s02, s03, g00, g01, sq3 = first_back(q0, k0, v0, do0, lse0, delta0, h0, by, wq, wk, wv, 0, False,
                                                    [add(3), add(4), share(3), share(3)], [c02, c03, s00, s01], side, 3)
        factor, g04, g02, g03, g14, _ = last([Job("both", 3), share(3), share(4), share(3)], [attn0, s02, s03, s14], [sq0, sq1, sq2, sq3],
                                             sum(w.size for w in weights), x.shape[2], side, 4)
        return adam(factor, weights, m, v, [[g00, g01, g02, g03, g04], [g10, g11, g12, g13, g14]])

    states, all_of = P(("rep", "dp"), None, None), P(None, None, None)
    return jax.shard_map(step, mesh=mesh, in_specs=(states, states) + (all_of,) * 21, out_specs=(P("rep", None, None),) * 21, check_vma=False)
```

```python
import argparse
import functools
import itertools

import jax
import jax.numpy as jnp
import numpy as np
from jax import lax
from jax.experimental import pallas as pl
from jax.experimental.pallas import tpu as pltpu
from jax.sharding import PartitionSpec as P

HEAD=128; THETA=10000
BF=jnp.bfloat16; F32=jnp.float32
VMEM = 56 * 2**20
LOG2E = 1.4426950408889634
HUGE = -1e30

def _dot(a, b, ca=1, cb=0):
    return lax.dot_general(a, b, (((ca,), (cb,)), ((), ())), preferred_element_type=F32)

def _dot_t(a, b):
    return _dot(a, b, 1, 1)

def _get(ref):
    return ref[...]

def _loop(many, what):
    lax.fori_loop(0, many, lambda i, _: what(i), None)

def _each(copies, what):
    for one in copies:
        getattr(one, what)()

def _cut(refs, *sizes):
    refs = iter(refs)
    return [list(itertools.islice(refs, size)) for size in sizes] + [list(refs)]

def _params(*sem, limit=VMEM):
    return pltpu.CompilerParams(dimension_semantics=sem, vmem_limit_bytes=limit)

def turns(tokens, block):
    half = HEAD // 2
    speed = THETA ** (-np.arange(half) / half)
    def pair(places):
        angle = places[:, None] * speed
        return (np.concatenate([np.cos(angle)] * 2, 1).astype(np.float32), np.concatenate([np.sin(angle)] * 2, 1).astype(np.float32))
    return (*pair(np.arange(block)), *pair(np.arange(0, tokens, block)))

def _rms(h):
    wide = h.astype(F32)
    return wide, lax.rsqrt(jnp.mean(wide * wide, -1, keepdims=True) + 1e-6)

def _angles(i, cl, sl, ch, sh):
    c0, s0 = ch[pl.ds(i, 1), :], sh[pl.ds(i, 1), :]
    c = _get(cl) * c0 - _get(sl) * s0
    s = _get(sl) * c0 + _get(cl) * s0
    lane = lax.broadcasted_iota(jnp.int32, s.shape, 1)
    return c, jnp.where(lane < HEAD // 2, -s, s)

def _qkv(h_ref, wq, wk, wv, cl, sl, ch, sh, q_ref, k_ref, v_ref):
    i = pl.program_id(0)
    wide, scale = _rms(_get(h_ref))
    a = (wide * scale).astype(BF)
    c, s = _angles(i, cl, sl, ch, sh)
    for w, out in ((wq, q_ref), (wk, k_ref)):
        t = _dot(a, _get(w)).astype(BF).astype(F32)
        for n in range(0, t.shape[1], HEAD):
            one = t[:, n:n+HEAD]
            out[:, n:n+HEAD] = (one * c + pltpu.roll(one, HEAD//2, 1) * s).astype(BF)
    v_ref[...] = _dot(a, _get(wv)).astype(BF)

def _weight(w, layer):
    return pl.BlockSpec((None, *w.shape[1:]), lambda *_: (layer, 0, 0), pipeline_mode=pl.Buffered(1))

def qkv(h, wq, wk, wv, layer, block=512):
    t, d = h.shape
    tables = turns(t, block)
    rows = pl.BlockSpec((block, d), lambda i: (i, 0))
    whole = lambda a: pl.BlockSpec(a.shape, lambda i: (0, 0), pipeline_mode=pl.Buffered(1))
    outs = [w.shape[2] for w in (wq, wk, wv)]
    return pl.pallas_call(_qkv, grid=(t // block,),
        in_specs=[rows, *(_weight(w, layer) for w in (wq, wk, wv)), *(whole(a) for a in tables)],
        out_specs=[pl.BlockSpec((block, n), lambda i: (i, 0)) for n in outs],
        out_shape=[jax.ShapeDtypeStruct((t, n), BF) for n in outs],
        compiler_params=_params("arbitrary"),
        cost_estimate=pl.CostEstimate(flops=2*t*d*sum(outs), bytes_accessed=2*t*(d+sum(outs)), transcendentals=0),
        name="qkv")(h, wq, wk, wv, *(jnp.asarray(a) for a in tables))

def _ffn(o_ref, h_ref, wo, wg, wu, wd, out_ref, *, wide):
    h1 = (_get(h_ref).astype(F32) + _dot(_get(o_ref), _get(wo)).astype(BF).astype(F32)).astype(BF)
    x, scale = _rms(h1)
    b = (x * scale).astype(BF)
    total = None
    for c in range(0, wg.shape[1], wide):
        gate = _dot(b, wg[:, c:c+wide])
        up = _dot(b, wu[:, c:c+wide])
        act = (gate * lax.logistic(gate) * up).astype(BF)
        one = _dot(act, wd[c:c+wide, :])
        total = one if total is None else total + one
    out_ref[...] = (h1.astype(F32) + total.astype(BF).astype(F32)).astype(BF)

def ffn(o, h, wo, wg, wu, wd, layer, block=512, wide=512):
    t, d = h.shape
    rows = lambda n: pl.BlockSpec((block, n), lambda i: (i, 0))
    return pl.pallas_call(functools.partial(_ffn, wide=wide), grid=(t // block,),
        in_specs=[rows(o.shape[1]), rows(d), *(_weight(w, layer) for w in (wo, wg, wu, wd))],
        out_specs=rows(d), out_shape=jax.ShapeDtypeStruct((t, d), BF),
        compiler_params=_params("arbitrary"),
        cost_estimate=pl.CostEstimate(flops=2*t*(d*o.shape[1]+3*d*wg.shape[2]), bytes_accessed=6*t*d, transcendentals=0),
        name="ffn")(o, h, wo, wg, wu, wd)


def _attend_s(q_ref, k_new, v_ref, o_ref, lse_ref, vt_s, top_s, mix_s, k_ref, *, heads, bq, scale):
    iq = pl.program_id(0)
    e = scale * LOG2E
    half = bq // 2
    cols = [pl.ds(n * HEAD, HEAD) for n in range(heads)]
    cut = [pl.ds(n * (HEAD + 8), HEAD + 8) for n in range(heads)]
    mine = pl.ds(pl.multiple_of(iq * bq, bq), bq)
    for n, c in enumerate(cols):
        vt_s[n * (HEAD + 8):n * (HEAD + 8) + HEAD, mine] = v_ref[:, c].T
        vt_s[n * (HEAD + 8) + HEAD:(n + 1) * (HEAD + 8), mine] = jnp.ones((8, bq), BF)
    k_ref[mine, :] = _get(k_new)
    top_s[...] = jnp.full_like(top_s, HUGE)
    mix_s[...] = jnp.zeros_like(mix_s)

    def block(at, size, pieces, ok):
        here, lane = pl.ds(at, size), pl.ds(pl.multiple_of(at, 128), size)
        scores = [_dot_t(k_ref[here, cols[n]], q_ref[a:a+w, cols[n]]) for n, a, w in pieces]
        ps, keeps = [], []
        for (n, a, w), s in zip(pieces, scores):
            if ok is not None:
                s = jnp.where(ok, s, 2 * HUGE)
            old = top_s[n:n+1, a:a+w]
            new = jnp.maximum(old, s.max(axis=0, keepdims=True))
            top_s[n:n+1, a:a+w] = new
            ps.append(jnp.exp2((s - new) * e).astype(BF))
            keeps.append(jnp.exp2((old - new) * e))
        for (n, a, w), p, keep in zip(pieces, ps, keeps):
            mix_s[cut[n], a:a+w] = mix_s[cut[n], a:a+w] * keep + _dot(vt_s[cut[n], lane], p)
    _loop(iq, lambda j: block(j * bq, bq, [(n, 0, bq) for n in range(heads)], None))
    seen = lambda w: lax.broadcasted_iota(jnp.int32, (half, w), 1) >= lax.broadcasted_iota(jnp.int32, (half, w), 0)
    block(iq * bq, half, [(n, 0, bq) for n in range(heads)], seen(bq))
    block(iq * bq + half, half, [(n, half, half) for n in range(heads)], seen(half))
    for n, c in enumerate(cols):
        total = mix_s[n * (HEAD + 8) + HEAD:n * (HEAD + 8) + HEAD + 1, :]
        o_ref[:, c] = (mix_s[n * (HEAD + 8):n * (HEAD + 8) + HEAD, :] * (1 / total)).T.astype(BF)
        lse_ref[n:n+1, :] = top_s[n:n+1, :] * e + jnp.log2(total)

def attend(q, k, v, bq=512):
    t, w = q.shape
    heads = w // HEAD
    rows = pl.BlockSpec((bq, w), lambda i: (i, 0))
    return pl.pallas_call(functools.partial(_attend_s, heads=heads, bq=bq, scale=HEAD**-0.5), grid=(t // bq,),
        in_specs=[rows] * 3,
        out_specs=[rows, pl.BlockSpec((heads, bq), lambda i: (0, i))],
        out_shape=[jax.ShapeDtypeStruct((t, w), BF), jax.ShapeDtypeStruct((heads, t), F32)],
        scratch_shapes=[pltpu.VMEM((heads * (HEAD + 8), t), BF), pltpu.VMEM((heads, bq), F32), pltpu.VMEM((heads * (HEAD + 8), bq), F32), pltpu.VMEM((t, w), BF)],
        compiler_params=_params("arbitrary"),
        cost_estimate=pl.CostEstimate(flops=2*t*t*w, bytes_accessed=8*t*w, transcendentals=heads*t*t//2), name="attend")(q, k, v)


MESH = pl.DeviceIdType.MESH

class Ring:
    def __init__(self, side):
        self.side, self.me = side, lax.axis_index("dp")
        at = self.me // side, self.me % side
        self.places = [[lax.rem(place + k, side) for k in range(side)] for place in at]

    def place(self, axis, away=0):
        return self.places[axis][away % self.side]

    def next(self, axis, sign):
        x, y = (self.place(n, sign if n == axis else 0) for n in range(2))
        return x * self.side + y

    def greet(self, far):
        many = self.side**2
        peers = [lax.rem(self.me + k, many) for k in range(1, many)] if far else [self.next(c // 2, _sign(c)) for c in range(4)]
        for peer in peers:
            pl.semaphore_signal(pltpu.get_barrier_semaphore(), inc=1, device_id={"dp": peer}, device_id_type=MESH)
        return peers


def _sign(c):
    return 1 - c % 2 * 2


def _four(what, many=4):
    for c in range(many):
        what(c)


def _send(src, dst, send, recv, to):
    return pltpu.make_async_remote_copy(src_ref=src, dst_ref=dst, send_sem=send, recv_sem=recv, device_id={"dp": to}, device_id_type=MESH)


def _rows(ref, at, size):
    return ref.at[:, pl.ds(pl.multiple_of(at, size), size), :]


class Scatter:
    steps = 4

    def __init__(self, ring, own, buffers, send, recv, result):
        self.ring, self.own, self.send, self.recv, self.result = ring, own, send, recv, result
        self.xa, self.xb, self.ya_out, self.ya, self.yb_out, self.yb = buffers
        self.big, self.small = self.xb.shape[-2], self.yb.shape[-2]

    def mine(self, c, part, rows, size):
        return _rows(self.own.at[c // 2], self.ring.place(c // 2, part) * self.big + rows, size)

    def copies(self, c, s):
        sign, axis = _sign(c), (c // 2 + s // 2) % 2
        half = self.big // 2
        rows, other = c % 2 * half, (1 - c % 2) * half
        if s == 0:
            pairs = [(self.mine(c, 2, rows, half), self.xa.at[c])]
        elif s == 1:
            pairs = [(self.xa.at[c], _rows(self.xb.at[c], rows, half)), (self.mine(c, sign, other, half), _rows(self.xb.at[c], other, half))]
        else:
            pairs = [(self.ya_out.at[c], self.ya.at[c]) if s == 2 else (self.yb_out.at[c], self.yb.at[c])]
        return [_send(a, b, self.send, self.recv.at[s], self.ring.next(axis, sign)) for a, b in pairs]

    def total(self, half, part, rows, size):
        at = self.ring.place(1 - half, part) * self.small + rows
        got = [_get(_rows(self.xb.at[2 * half + n], at, size)).astype(F32) for n in range(2)]
        return got[0] + got[1] + _get(self.mine(2 * half, 0, at, size)).astype(F32)

    def ready(self, c, s):
        sign, half = _sign(c), self.small // 2
        rows = c % 2 * half
        if s == 1:
            self.xa[c] = (self.xa[c].astype(F32) + _get(self.mine(c, sign, c % 2 * (self.big // 2), self.big // 2)).astype(F32)).astype(BF)
        elif s == 2:
            self.ya_out[c] = self.total(c // 2, 2, rows, half).astype(BF)
        elif s == 3:
            _rows(self.yb_out.at[c], half - rows, half)[...] = self.total(c // 2, sign, half - rows, half).astype(BF)
            _rows(self.yb_out.at[c], rows, half)[...] = (self.total(c // 2, sign, rows, half) + self.ya[c].astype(F32)).astype(BF)

    def sent(self):
        same = self.own.at[:, :, pl.ds(0, 3 * (self.big + self.small)), :]
        _send(same, same, self.send, self.recv.at[0], self.ring.me).wait_send()

    def step(self, s):
        if s:
            got = (self.xa, self.xb, self.ya, self.yb)[s - 1]
            _send(got, got, self.send, self.recv.at[s - 1], self.ring.me).wait_recv()
        if s == self.steps:
            def close(half):
                total = self.total(half, 0, 0, self.small)
                self.result(half)[...] = (total + self.yb[2 * half].astype(F32) + self.yb[2 * half + 1].astype(F32)).astype(BF)
            _four(close, 2)
            return
        if s:
            _four(lambda c: self.ready(c, s))
        _four(lambda c: [one.start() for one in self.copies(c, s)])


class Gather:
    steps = 4

    def __init__(self, ring, whole, send, recv, base):
        self.ring, self.whole, self.send, self.recv, self.base = ring, whole, send, recv, base
        self.big = whole.shape[-2] // ring.side

    def place(self, half):
        small = self.big // self.ring.side
        return _rows(self.whole.at[half], self.ring.place(half) * self.big + self.ring.place(1 - half) * small, small)

    def copies(self, c, s):
        ring, sign, half = self.ring, _sign(c), c // 2
        axis = (1 - half) if s < 2 else half
        size = self.big // ring.side if s < 2 else self.big
        far = s % 2
        at = ring.place(axis, -sign * far) * size + far * (c % 2) * (size // 2)
        if s < 2:
            at = ring.place(half) * self.big + at
        part = _rows(self.whole.at[half], at, size // (1 + far))
        return _send(part, part, self.send, self.recv.at[self.base + s], ring.next(axis, sign))

    def step(self, s):
        if s:
            self.same((self.big if s > 2 else self.big // self.ring.side) * (1 + s % 2), s - 1).wait_recv()
        if s < self.steps:
            _four(lambda c: self.copies(c, s).start())

    def same(self, rows, s):
        part = self.whole.at[:, :, pl.ds(0, rows), :]
        return _send(part, part, self.send, self.recv.at[self.base + s], self.ring.me)

    def sent(self):
        self.same(3 * (self.big + self.big // self.ring.side), 0).wait_send()


class Job:
    def __init__(self, kind, matrices, time=1.0, made=False):
        self.kind, self.matrices, self.time, self.made, self.first, self.many = kind, matrices, time, made, 0, matrices
        self.sums, self.shares = kind != "share", kind != "sum"

    def sizes(self):
        return [self.matrices * BIG * k for k in ([0.5, 1, 0.125, 0.25] * self.sums + [0.25, 0.125, 1, 0.5] * self.shares)]


BIG, LAG = 1.43, 2.5


def plan(jobs, times):
    wire, state, out = 0.0, [(0, job.time) for job in jobs], []
    now = 0.0
    def advance():
        nonlocal wire
        picks = []
        for j, job in enumerate(jobs):
            s, ready = state[j]
            sizes = job.sizes()
            if s <= len(sizes) and ready <= now:
                picks.append((j, s))
                if s < len(sizes):
                    wire = max(wire, now) + sizes[s]
                state[j] = (s + 1, wire + LAG)
        return picks
    for now in times:
        out.append(advance())
    rest = []
    while todo := [ready for (s, ready), job in zip(state, jobs) if s <= len(job.sizes())]:
        now = max(now, min(todo))
        rest += advance()
    return out + [rest]


class Traffic:
    def __init__(self, jobs, side, rows, times, far=False):
        self.jobs, self.side, self.rows, self.far = jobs, side, rows, far
        self.plan = plan(jobs, times)
        small = rows // side**2
        hbm, vmem = pl.BlockSpec(memory_space=pltpu.HBM), lambda *s: pl.BlockSpec(s, lambda *_: (0,) * len(s), pipeline_mode=pl.Buffered(1))
        self.in_specs, self.out_specs, self.out_shape, self.scratch = [], [], [], []
        for job in jobs:
            unit = lambda many, size: (many, job.matrices, size, rows // 2)
            if not job.made:
                self.in_specs.append(hbm if job.sums else vmem(*unit(2, small)))
            if job is not jobs[0] and job.made:
                job.first = jobs[0].many
                jobs[0].many += job.matrices
            else:
                self.out_specs.append(hbm if job.shares else vmem)
                self.out_shape.append((job, rows if job.shares else small))
            if job.sums:
                sizes = (rows // side // 2, rows // side, small // 2, small // 2, small, small)
                self.scratch += [pltpu.VMEM(unit(2, rows), BF)] * (not job.made) + [pltpu.VMEM(unit(4, size), BF) for size in sizes]
            if job.shares:
                self.scratch.append(pltpu.VMEM(unit(2, rows), BF))
            self.scratch += [pltpu.SemaphoreType.DMA((2,)), pltpu.SemaphoreType.DMA((len(job.sizes()),)), pltpu.SemaphoreType.DMA((2,))]
        self.out_shape = [jax.ShapeDtypeStruct((2, job.many, size, rows // 2), BF) for job, size in self.out_shape] + [jax.ShapeDtypeStruct((8, HEAD), F32)]
        self.out_specs = [spec if spec is hbm else vmem(*a.shape) for spec, a in zip(self.out_specs + [vmem], self.out_shape)]

    def bind(self, ins, outs, scratch, made=()):
        ins, outs, scratch, made = iter(ins), iter(outs), iter(scratch), iter(made)
        self.ring = Ring(self.side)
        self.run, self.mine = [], []
        for job in self.jobs:
            r = argparse.Namespace(given=None if job.made else next(ins), out=self.run[0].out if job.first else next(outs))
            if job.sums:
                r.own = next(made) if job.made else next(scratch)
                buffers = [next(scratch) for _ in range(6)]
            if job.shares:
                r.whole = next(scratch)
            send, recv, sem = (next(scratch) for _ in range(3))
            if job.shares:
                r.gather = Gather(self.ring, r.whole, send.at[1], recv, Scatter.steps * job.sums)
                r.store = pltpu.make_async_copy(r.whole, r.out, sem.at[1])
            if job.sums:
                r.scatter = Scatter(self.ring, r.own, buffers, send.at[0], recv, r.gather.place if job.shares else lambda half, r=r, job=job: r.out.at[half, pl.ds(job.first, job.matrices)])
                r.load = None if job.made else pltpu.make_async_copy(r.given, r.own, sem.at[0])
            self.run.append(r)
        self.squares = next(outs)

    def start(self):
        for job, r in zip(self.jobs, self.run):
            if job.sums and not job.made:
                r.load.start()
        self.squares[...] = jnp.zeros_like(self.squares)
        self.peers = self.ring.greet(self.far)

    def meet(self):
        pl.semaphore_wait(pltpu.get_barrier_semaphore(), len(self.peers))

    def take(self, j, s):
        job, r = self.jobs[j], self.run[j]
        steps = Scatter.steps
        if s == 0 and not job.made and job.sums:
            r.load.wait()
        if job.sums and s <= steps:
            r.scatter.step(s)
            if s == steps:
                def fold(c):
                    got = r.scatter.result(c)[...].astype(F32)
                    got = (got * got).reshape(-1, 8, got.shape[-1]).sum(0)
                    self.squares[...] += sum(got[:, n:n + HEAD] for n in range(0, got.shape[-1], HEAD))
                _four(fold, 2)
        if job.shares and s >= steps * job.sums:
            if not job.sums and s == 0:
                def put(c):
                    r.gather.place(c)[...] = r.given[c]
                _four(put, 2)
            r.gather.step(s - steps * job.sums)
            if s == steps * (1 + job.sums):
                r.store.start()

    def tick(self, now, possible):
        for n in possible:
            picks = self.plan[n]
            if picks:
                @pl.when(now == n)
                def _():
                    for j, s in picks:
                        self.take(j, s)

    def finish(self):
        for j, s in self.plan[-1]:
            self.take(j, s)
        for job, r in zip(self.jobs, self.run):
            for part in ([r.scatter] if job.sums else []) + ([r.gather] if job.shares else []):
                part.sent()
            if job.shares:
                r.store.wait()


def _once(*shape):
    return pl.BlockSpec(shape, lambda *_: (0,) * len(shape), pipeline_mode=pl.Buffered(1))

def _comm(ident):
    return pltpu.CompilerParams(dimension_semantics=("arbitrary",), vmem_limit_bytes=MOST, collective_id=ident, has_side_effects=True)

MOST = 63 * 2**20

def _norm_back(x, s, by):
    by = by.astype(BF).astype(F32)
    return (s * by - x * (s * s * s * jnp.mean(by * x, -1, keepdims=True))).astype(BF).astype(F32)


def _split(to, value):
    for half, part in enumerate(jnp.split(value, 2, 1)):
        to(half)[...] = part.astype(BF)

def _half(*refs, block, sub, traffic, n_in, n_out, early):
    main, ins, rest, mine, outs, own, scratch = _cut(refs, 7, n_in, 1, 3, n_out, 16)
    *whole, wo, wg, wu, wd = main
    do_ref, delta_ref, dh_ref = mine
    h1_s, b_s, bt_s, dyt_s, act_s, dg_s, du_s, db_s, own_s, own_sem, o_ref, h_ref, dy_ref, do_s, sem, out_sem = own
    dh_s = h_ref
    c, last = pl.program_id(0), own_s.shape[0] - 1
    t, d = h_ref.shape
    per = t // block
    units = [own_s.at[n, :, pl.ds(0, 3)] for n in range(last)] + [own_s.at[last]]
    traffic.bind(ins, outs, scratch, units[:early])
    keep = [pltpu.make_async_copy(unit, rest[0].at[:, pl.ds(3 * n, unit.shape[1])], own_sem.at[n]) for n, unit in enumerate(units[early:])]
    at = lambda i: pl.ds(pl.multiple_of(i * block, block), block)
    loads = lambda i: [pltpu.make_async_copy(a.at[at(i), :], b.at[at(i), :], sem.at[n, i]) for n, (a, b) in enumerate(zip(whole, (o_ref, h_ref, dy_ref)))]
    stores = lambda i: [pltpu.make_async_copy(a.at[at(i), :], b.at[at(i), :], out_sem.at[n, i]) for n, (a, b) in enumerate(((do_s, do_ref), (dh_s, dh_ref)))]

    @pl.when(c == 0)
    def _():
        _loop(per, lambda i: _each(loads(i), "start"))
        traffic.start()
        def head(i):
            _each(loads(i), "wait")
            h1 = (h_ref[at(i), :].astype(F32) + _dot(o_ref[at(i), :], _get(wo)).astype(BF).astype(F32)).astype(BF)
            h1_s[at(i), :] = h1
            x, scale = _rms(h1)
            b = (x * scale).astype(BF)
            b_s[at(i), :] = b
            bt_s[:, at(i)] = b.T
            dyt_s[:, at(i)] = dy_ref[at(i), :].T
            db_s[at(i), :] = jnp.zeros((block, d), F32)
        _loop(per, head)
        traffic.meet()

    def body(i):
        traffic.tick(c * (per + 3) + i, [n for n in range((last + 1) * (per + 3)) if n % (per + 3) < per])
        rows = [pl.ds(i * block + k, sub) for k in range(0, block, sub)]
        first = [(_dot(b_s[r, :], _get(wg)), _dot(b_s[r, :], _get(wu)), _dot_t(dy_ref[r, :], _get(wd))) for r in rows]
        for r, (gate, up, dact) in zip(rows, first):
            dact = dact.astype(BF).astype(F32)
            sig = lax.logistic(gate)
            silu = gate * sig
            act_s[r, :] = (silu * up).astype(BF)
            du = (dact * silu).astype(BF)
            dg = (dact * up * (sig + silu * (1 - sig))).astype(BF)
            du_s[r, :] = du
            dg_s[r, :] = dg
            db_s[r, :] += _dot_t(dg, _get(wg)) + _dot_t(du, _get(wu))
    _loop(per, body)
    for m, value in enumerate((lambda: _dot(_get(bt_s), _get(dg_s)), lambda: _dot(_get(bt_s), _get(du_s)), lambda: _dot(_get(dyt_s), _get(act_s)).T)):
        traffic.tick(c * (per + 3) + per + m, range(per + m, (last + 1) * (per + 3), per + 3))
        _split(lambda k: own_s.at[c, k, m], value())
    for n, one in enumerate(keep[:-1]):
        pl.when(c == early + n)(one.start)

    @pl.when(c == last)
    def _():
        def tail(i):
            traffic.tick((last + 1) * (per + 3) + i, range((last + 1) * (per + 3), len(traffic.plan) - 1))
            x, s = _rms(h1_s[at(i), :])
            dh = (dy_ref[at(i), :].astype(F32) + _norm_back(x, s, db_s[at(i), :])).astype(BF)
            dh_s[at(i), :] = dh
            do = _dot_t(dh, _get(wo)).astype(BF)
            do_s[at(i), :] = do
            _each(stores(i), "start")
            prod = do.astype(F32) * o_ref[at(i), :].astype(F32)
            lane = lax.broadcasted_iota(jnp.int32, (block, HEAD), 1)
            sums = jnp.zeros((block, HEAD), F32)
            for n in range(prod.shape[1] // HEAD):
                sums = jnp.where(lane == n, prod[:, n*HEAD:(n+1)*HEAD].sum(-1, keepdims=True), sums)
            delta_ref[:, at(i)] = sums.T[:delta_ref.shape[0], :]
        _loop(per, tail)
        _split(lambda k: own_s.at[last, k, 3], _dot(_get(o_ref), _get(dh_s), 0, 0))
        keep[-1].start()
        traffic.finish()
        _each(keep, "wait")
        _loop(per, lambda i: _each(stores(i), "wait"))

def half_back(o, h, dy, wo, wg, wu, wd, layer, early, jobs, given, side, ident, block=512, sub=256, start=5.5, pace=1.75, dots=1.15, slow=1.3):
    t, d = h.shape
    e, f = o.shape[1], wg.shape[2]
    chunks, per = f // d, t // block
    times = []
    for c in range(chunks):
        now = start + c * (pace * per + dots * 3)
        times += [now + pace * i for i in range(per)] + [now + pace * per + dots * i for i in range(3)]
    times += [start + chunks * (pace * per + dots * 3) + slow * i for i in range(per)]
    made = [Job("sum", 3, start + (c + 1) * (pace * per + dots * 3), True) for c in range(early)]
    rest = jax.ShapeDtypeStruct((2, 3 * (chunks - early) + 1, d, d // 2), BF)
    traffic = Traffic(made + jobs, side, d, times)
    col, row = pl.BlockSpec((None, d, d), lambda c: (layer, 0, c)), pl.BlockSpec((None, d, d), lambda c: (layer, c, 0))
    big, hbm = lambda kind: pltpu.VMEM((t, d), kind), pl.BlockSpec(memory_space=pltpu.HBM)
    return pl.pallas_call(functools.partial(_half, block=block, sub=sub, traffic=traffic, n_in=len(given), n_out=len(traffic.out_specs), early=early), grid=(chunks,),
        in_specs=[hbm] * 3 + [_weight(wo, layer), col, col, row, *traffic.in_specs],
        out_specs=[hbm, hbm, _once(e // HEAD, t), hbm, *traffic.out_specs],
        out_shape=[rest, jax.ShapeDtypeStruct((t, e), BF), jax.ShapeDtypeStruct((e // HEAD, t), F32),
                   jax.ShapeDtypeStruct((t, d), BF), *traffic.out_shape],
        scratch_shapes=[big(BF), big(BF), pltpu.VMEM((d, t), BF), pltpu.VMEM((d, t), BF), big(BF), big(BF), big(BF), big(F32),
                        pltpu.VMEM((chunks, 2, 4, d, d // 2), BF), pltpu.SemaphoreType.DMA((chunks,)), *[big(BF)] * 4, *[pltpu.SemaphoreType.DMA((3, per))] * 2, *traffic.scratch],
        compiler_params=_comm(ident),
        cost_estimate=pl.CostEstimate(flops=2*t*(3*d*e+8*d*f), bytes_accessed=12*t*d, transcendentals=0),
        name="half_back")(o, h, dy, wo, wg, wu, wd, *given)

def _first(*refs, heads, bq, scale, deep, layer, traffic, n_in, n_out):
    main, late, ins, (unit_ref,), dx_ref, outs, own, held, scratch = _cut(refs, 11, 4 * deep, n_in, 1, deep, n_out, 10, 6 * deep)
    q_ref, k_new, v_new, do_ref, lse_ref, delta_ref, h_ref, cl, sl, ch, sh = main
    kt_s, dq_s, dk_s, dv_s, q_s, at_s, k_s, v_s, k_ref, v_ref = own
    loads = []
    if deep:
        h_s, dh_s, wq, wk, wv, sem = held
        loads = [pltpu.make_async_copy(a if n == 0 else a.at[layer], b, sem.at[n]) for n, (a, b) in enumerate(zip(late, held[1:]))]
    iq, last = pl.program_id(0), k_ref.shape[0] // bq - 1
    e = scale * LOG2E
    half = bq // 2
    cols = [pl.ds(n * HEAD, HEAD) for n in range(heads)]
    at = lambda i: pl.ds(pl.multiple_of(i * bq, bq), bq)
    mine = at(iq)
    traffic.bind(ins, outs, scratch)

    @pl.when(iq == 0)
    def _():
        traffic.start()
        _each(loads, "start")
    x, s = _rms(_get(h_ref))
    at_s[:, mine] = (x * s).astype(BF).T
    if deep:
        h_s[mine, :] = _get(h_ref)
    k_ref[mine, :] = _get(k_new)
    v_ref[mine, :] = _get(v_new)
    for c in cols:
        kt_s[c, mine] = k_new[:, c].T
    dq_s[...] = jnp.zeros_like(dq_s)
    dk_s[mine, :] = jnp.zeros((bq, k_ref.shape[1]), F32)
    dv_s[mine, :] = jnp.zeros((bq, k_ref.shape[1]), F32)

    def block(at, size, pieces, ok):
        here, lane = pl.ds(at, size), pl.ds(pl.multiple_of(at, HEAD), size)
        scores = [_dot_t(k_ref[here, cols[n]], q_ref[a:a+w, cols[n]]) for n, a, w in pieces]
        dps = [_dot_t(v_ref[here, cols[n]], do_ref[a:a+w, cols[n]]) for n, a, w in pieces]
        for (n, a, w), s, dp in zip(pieces, scores, dps):
            p = jnp.exp2(s * e - lse_ref[n:n+1, a:a+w])
            if ok is not None:
                p = jnp.where(ok, p, 0.0)
            ds = (p * (dp - delta_ref[n:n+1, a:a+w])).astype(BF)
            dv_s[here, cols[n]] += _dot(p.astype(BF), do_ref[a:a+w, cols[n]])
            dk_s[here, cols[n]] += _dot(ds, q_ref[a:a+w, cols[n]])
            dq_s[cols[n], a:a+w] += _dot(kt_s[cols[n], lane], ds)

    pl.when(iq == 0)(traffic.meet)
    before = iq * (iq + 1) // 2
    cuts = list(itertools.accumulate(range(1, last + 2), initial=0))
    *cuts, ticks = [n for n in cuts[:-1]] + [cuts[-1]]
    cuts = [n + k for k, n in enumerate(cuts)]
    def off(j):
        traffic.tick(before + j, [n for n in range(ticks) if n not in cuts])
        block(j * bq, bq, [(n, 0, bq) for n in range(heads)], None)
    _loop(iq, off)
    traffic.tick(before + iq, cuts)
    seen = lambda w: lax.broadcasted_iota(jnp.int32, (half, w), 1) >= lax.broadcasted_iota(jnp.int32, (half, w), 0)
    block(iq * bq, half, [(n, 0, bq) for n in range(heads)], seen(bq))
    block(iq * bq + half, half, [(n, half, half) for n in range(heads)], seen(half))

    def unturned(i, value):
        c, s = _angles(i, cl, sl, ch, sh)
        one = (value * scale).astype(BF).astype(F32)
        return (one * c - pltpu.roll(one, HEAD // 2, 1) * s).astype(BF)
    for c in cols:
        q_s[mine, c] = unturned(iq, dq_s[c, :].T)

    @pl.when(iq == last)
    def _():
        _each(loads, "wait")
        def tail(i):
            traffic.tick(ticks + i, range(ticks, ticks + last + 1))
            for c in cols:
                k_s[at(i), c] = unturned(i, dk_s[at(i), c])
            v_s[at(i), :] = dv_s[at(i), :].astype(BF)
            if deep:
                by = _dot_t(q_s[at(i), :], _get(wq)) + _dot_t(k_s[at(i), :], _get(wk)) + _dot_t(v_s[at(i), :], _get(wv))
                x, s = _rms(h_s[at(i), :])
                dx_ref[0][at(i), :] = (dh_s[at(i), :].astype(F32) + _norm_back(x, s, by)).astype(BF)
        _loop(last + 1, tail)
        for m, value in enumerate((q_s, k_s, v_s)):
            traffic.tick(ticks + last + 1 + m, [ticks + last + 1 + m])
            _split(lambda k: unit_ref.at[k, m], _dot(_get(at_s), _get(value)))
        traffic.finish()


def first_back(q, k, v, do, lse, delta, h, dh, wq, wk, wv, layer, deep, jobs, given, side, ident, bq=512, start=2.0, pace=3.5, more=3.2, end=1.3):
    t, w = q.shape
    d, heads = h.shape[1], w // HEAD
    now, times = start, []
    for i in range(t // bq):
        times += [now + pace * j for j in range(i + 1)]
        now += pace * i + more
    times += [now + end * i for i in range(t // bq + 3)]
    traffic = Traffic(jobs, side, d, times)
    rows, stats = pl.BlockSpec((bq, w), lambda i: (i, 0)), pl.BlockSpec((heads, bq), lambda i: (0, i))
    tables = [jnp.asarray(a) for a in turns(t, bq)]
    big = lambda kind: pltpu.VMEM((t, w), kind)
    late = [dh, wq, wk, wv] * deep
    held = [pltpu.VMEM((t, d), BF)] * 2 * deep + [pltpu.VMEM(m.shape[1:], BF) for m in late[1:]] + [pltpu.SemaphoreType.DMA((len(late),))] * deep
    return pl.pallas_call(functools.partial(_first, heads=heads, bq=bq, scale=HEAD**-0.5, deep=deep, layer=layer, traffic=traffic, n_in=len(given), n_out=len(traffic.out_specs)),
        grid=(t // bq,),
        in_specs=[rows] * 4 + [stats, stats, pl.BlockSpec((bq, d), lambda i: (i, 0)), *(_once(*a.shape) for a in tables),
                  *[pl.BlockSpec(memory_space=pltpu.HBM)] * len(late), *traffic.in_specs],
        out_specs=[_once(2, 3, d, d // 2)] + [_once(t, d)] * deep + traffic.out_specs,
        out_shape=[jax.ShapeDtypeStruct((2, 3, d, d // 2), BF)] + [jax.ShapeDtypeStruct((t, d), BF)] * deep + traffic.out_shape,
        scratch_shapes=[pltpu.VMEM((w, t), BF), pltpu.VMEM((w, bq), F32), big(F32), big(F32), big(BF), pltpu.VMEM((d, t), BF), *[big(BF)] * 4, *held, *traffic.scratch],
        compiler_params=_comm(ident),
        cost_estimate=pl.CostEstimate(flops=5*t*t*w, bytes_accessed=14*t*w, transcendentals=heads*t*t//2),
        name="first_back")(q, k, v, do, lse, delta, h, *tables, *late, *given)

def _last(*refs, traffic, n_in, n_out, known, count):
    ins, known, (factor_ref,), outs, (sums_s, one_s, send, recv), scratch = _cut(refs, n_in, known, 1, n_out, 4)
    traffic.bind(ins, outs, scratch)
    traffic.start()
    traffic.meet()
    me, n = traffic.ring.me, traffic.side**2
    copy = lambda peer, slot: _send(one_s, sums_s.at[slot], send.at[lax.rem(peer - me + n, n)], recv.at[slot], peer)
    waiting = sum(job.sums for job in traffic.jobs)
    for j, s in traffic.plan[-1]:
        traffic.take(j, s)
        if traffic.jobs[j].sums and s == Scatter.steps:
            waiting -= 1
            if not waiting:
                one_s[...] = sum((_get(ref) for ref in known), _get(traffic.squares))
                sums_s[me] = _get(one_s)
                for peer in traffic.peers:
                    copy(peer, me).start()
    traffic.plan[-1].clear()
    for peer in traffic.peers:
        copy(peer, peer).wait_recv()
    total = sums_s[0]
    for k in range(1, n):
        total = total + sums_s[k]
    factor_ref[...] = jnp.broadcast_to(jnp.minimum(1.0, 0.5 * lax.rsqrt(jnp.sum(total, keepdims=True) / count + 1e-30)), factor_ref.shape)
    for peer in traffic.peers:
        copy(peer, me).wait_send()
    traffic.finish()

def last(jobs, given, known, count, rows, side, ident):
    traffic = Traffic(jobs, side, rows, [], True)
    tile = jax.ShapeDtypeStruct((8, HEAD), F32)
    n = side**2
    return pl.pallas_call(functools.partial(_last, traffic=traffic, n_in=len(given), n_out=len(traffic.out_specs), known=len(known), count=count), grid=(1,),
        in_specs=traffic.in_specs + [_once(*tile.shape)] * len(known), out_specs=[_once(*tile.shape)] + traffic.out_specs, out_shape=[tile] + traffic.out_shape,
        scratch_shapes=[pltpu.VMEM((n, *tile.shape), F32), pltpu.VMEM(tile.shape, F32), *[pltpu.SemaphoreType.DMA((n,))] * 2, *traffic.scratch],
        compiler_params=_comm(ident), name="last")(*given, *known)

def _adam(*refs, arrays, units, places, slots, ahead, piece):
    (factor_ref,), w, m, v, g, new, (w_s, m_s, v_s, g_s, load, store) = _cut(refs, 1, *[arrays] * 3, units, 3 * arrays)
    factor = factor_ref[:1, :1]
    d = w_s.shape[2]

    def loads(i):
        array, layer, row, col, unit, matrix, part = places[i]
        k = i % slots
        spot = lambda a: a.at[layer, pl.ds(row, piece), pl.ds(col, d)]
        pairs = [(spot(a[array]), b.at[k]) for a, b in ((w, w_s), (m, m_s), (v, v_s))] + [(g[unit].at[:, matrix, pl.ds(part, piece), :], g_s.at[k])]
        return [pltpu.make_async_copy(a, b, load.at[k, n]) for n, (a, b) in enumerate(pairs)]

    def stores(i):
        array, layer, row, col, *_ = places[i]
        k = i % slots
        return [pltpu.make_async_copy(a.at[k], new[n * arrays + array].at[layer, pl.ds(row, piece), pl.ds(col, d)], store.at[k, n])
                for n, a in enumerate((w_s, m_s, v_s))]

    for i in range(min(ahead, len(places))):
        _each(loads(i), "start")
    for i in range(len(places)):
        _each(loads(i), "wait")
        k = i % slots
        def update(r):
            rows = pl.ds(r * 32, 32)
            for c in range(2):
                cols = pl.ds(c * (d // 2), d // 2)
                grad = g_s[k, c, rows, :].astype(F32) * factor
                first = 0.9 * m_s[k, rows, cols] + 0.1 * grad
                second = 0.95 * v_s[k, rows, cols] + 0.05 * grad * grad
                old = w_s[k, rows, cols].astype(F32)
                m_s[k, rows, cols] = first
                v_s[k, rows, cols] = second
                w_s[k, rows, cols] = (old - 0.02 * (first * lax.rsqrt(second + 1e-8) + 0.1 * old)).astype(BF)
        _loop(piece // 32, update)
        _each(stores(i), "start")
        if i + ahead < len(places):
            if i + ahead >= slots:
                _each(stores(i + ahead - slots), "wait")
            _each(loads(i + ahead), "start")
    for i in range(max(len(places) - slots, 0), len(places)):
        _each(stores(i), "wait")

def adam(factor, w, m, v, units, slots=16, ahead=10, piece=256):
    d = w[0].shape[1]
    places, flat = [], []
    for layer, mine in reversed(list(enumerate(units))):
        spots = [(unit, matrix) for unit, a in enumerate(mine) for matrix in range(a.shape[1])]
        arrays = [(array, 0, n * d) if array < 6 else (array, n * d, 0) for n in range(w[4].shape[2] // d) for array in (4, 5, 6)] + [(i, 0, 0) for i in (3, 0, 1, 2)]
        places += [(array, layer, row + part, col, len(flat) + unit, matrix, part) for (array, row, col), (unit, matrix) in zip(arrays, spots) for part in range(0, d, piece)]
        flat += mine
    hbm = pl.BlockSpec(memory_space=pltpu.HBM)
    size = sum(a.size for a in w)
    return pl.pallas_call(functools.partial(_adam, arrays=len(w), units=len(flat), places=places, slots=slots, ahead=ahead, piece=piece), grid=(1,),
        in_specs=[_once(8, HEAD)] + [hbm] * (3 * len(w) + len(flat)), out_specs=[hbm] * (3 * len(w)),
        out_shape=[jax.ShapeDtypeStruct(a.shape, a.dtype) for a in (*w, *m, *v)],
        scratch_shapes=[pltpu.VMEM((slots, piece, d), BF), pltpu.VMEM((slots, piece, d), F32), pltpu.VMEM((slots, piece, d), F32), pltpu.VMEM((slots, 2, piece, d // 2), BF),
                        pltpu.SemaphoreType.DMA((slots, 4)), pltpu.SemaphoreType.DMA((slots, 3))],
        compiler_params=pltpu.CompilerParams(dimension_semantics=("arbitrary",), vmem_limit_bytes=VMEM),
        cost_estimate=pl.CostEstimate(flops=16*size, bytes_accessed=22*size, transcendentals=size), name="adam")(factor, *w, *m, *v, *flat)


def solution(mesh):
    side = round(mesh.shape["dp"] ** 0.5)

    def step(x, dy, *arrays):
        weights, m, v = (arrays[i : i + 7] for i in (0, 7, 14))
        wq, wk, wv, wo, wg, wu, wd = weights
        h0 = x[0]
        q0, k0, v0 = qkv(h0, wq, wk, wv, 0)
        o0, lse0 = attend(q0, k0, v0)
        h1 = ffn(o0, h0, wo, wg, wu, wd, 0)
        q1, k1, v1 = qkv(h1, wq, wk, wv, 1)
        o1, lse1 = attend(q1, k1, v1)
        add, share = (lambda n, kind=kind: Job(kind, n) for kind in ("sum", "share"))
        late1, do1, delta1, by1, s10, sq0 = half_back(o1, h1, dy[0], wo, wg, wu, wd, 1, 3, [], [], side, 0)
        attn1, by0, s11, g10, sq1 = first_back(q1, k1, v1, do1, lse1, delta1, h1, by1, wq, wk, wv, 1, True, [add(4), share(9)], [late1, s10], side, 1)
        late0, do0, delta0, by, s00, g12, g11, sq2 = half_back(o0, h0, by0, wo, wg, wu, wd, 0, 3, [Job("both", 3), share(4)], [attn1, s11], side, 2)
        attn0, s01, g00, sq3 = first_back(q0, k0, v0, do0, lse0, delta0, h0, by, wq, wk, wv, 0, False, [add(4), share(9)], [late0, s00], side, 3)
        factor, g02, g01, _ = last([Job("both", 3), share(4)], [attn0, s01], [sq0, sq1, sq2, sq3],
                                        sum(w.size for w in weights), x.shape[2], side, 4)
        return adam(factor, weights, m, v, [[g00, g01, g02], [g10, g11, g12]])

    states, all_of = P(("rep", "dp"), None, None), P(None, None, None)
    return jax.shard_map(step, mesh=mesh, in_specs=(states, states) + (all_of,) * 21, out_specs=(P("rep", None, None),) * 21, check_vma=False)
```

```python
import argparse
import functools
import itertools

import jax
import jax.numpy as jnp
import numpy as np
from jax import lax
from jax.experimental import pallas as pl
from jax.experimental.pallas import tpu as pltpu
from jax.sharding import PartitionSpec as P

HEAD=128; THETA=10000
BF=jnp.bfloat16; F32=jnp.float32
VMEM = 56 * 2**20
LOG2E = 1.4426950408889634
HUGE = -1e30

def _dot(a, b, ca=1, cb=0):
    return lax.dot_general(a, b, (((ca,), (cb,)), ((), ())), preferred_element_type=F32)

def _dot_t(a, b):
    return _dot(a, b, 1, 1)

def _get(ref):
    return ref[...]

def _loop(many, what):
    lax.fori_loop(0, many, lambda i, _: what(i), None)

def _each(copies, what):
    for one in copies:
        getattr(one, what)()

def _cut(refs, *sizes):
    refs = iter(refs)
    return [list(itertools.islice(refs, size)) for size in sizes] + [list(refs)]

def _params(*sem, limit=VMEM):
    return pltpu.CompilerParams(dimension_semantics=sem, vmem_limit_bytes=limit)

def turns(tokens, block):
    half = HEAD // 2
    speed = THETA ** (-np.arange(half) / half)
    def pair(places):
        angle = places[:, None] * speed
        return (np.concatenate([np.cos(angle)] * 2, 1).astype(np.float32), np.concatenate([np.sin(angle)] * 2, 1).astype(np.float32))
    return (*pair(np.arange(block)), *pair(np.arange(0, tokens, block)))

def _rms(h):
    wide = h.astype(F32)
    return wide, lax.rsqrt(jnp.mean(wide * wide, -1, keepdims=True) + 1e-6)

def _angles(i, cl, sl, ch, sh):
    c0, s0 = ch[pl.ds(i, 1), :], sh[pl.ds(i, 1), :]
    c = _get(cl) * c0 - _get(sl) * s0
    s = _get(sl) * c0 + _get(cl) * s0
    lane = lax.broadcasted_iota(jnp.int32, s.shape, 1)
    return c, jnp.where(lane < HEAD // 2, -s, s)

def _weight(w, layer):
    return pl.BlockSpec((None, *w.shape[1:]), lambda *_: (layer, 0, 0), pipeline_mode=pl.Buffered(1))

def _forward(*refs, heads, bq, scale, second):
    before, (h_ref, wq, wk, wv, cl, sl, ch, sh), h1_ref, outs, own = _cut(refs, 5 * second, 8, second, 5)
    q_ref, k_ref, v_ref, o_ref, lse_ref = outs
    vt_s, top_s, mix_s, k_s = own
    iq = pl.program_id(0)
    e = scale * LOG2E
    half = bq // 2
    h = _get(h_ref)
    if second:
        last_ref, wo, wg, wu, wd = before
        h = (h.astype(F32) + _dot(_get(last_ref), _get(wo)).astype(BF).astype(F32)).astype(BF)
        x, s = _rms(h)
        b = (x * s).astype(BF)
        total = []
        for c in range(0, wg.shape[1], bq):
            gate = _dot(b, wg[:, c:c+bq])
            act = (gate * lax.logistic(gate) * _dot(b, wu[:, c:c+bq])).astype(BF)
            total.append(_dot(act, wd[c:c+bq, :]))
        h = (h.astype(F32) + functools.reduce(jnp.add, total).astype(BF).astype(F32)).astype(BF)
        h1_ref[0][...] = h
    x, s = _rms(h)
    a = (x * s).astype(BF)
    cos, sin = _angles(iq, cl, sl, ch, sh)
    cols = [pl.ds(n * HEAD, HEAD) for n in range(heads)]
    cut = [pl.ds(n * (HEAD + 8), HEAD + 8) for n in range(heads)]
    mine = pl.ds(pl.multiple_of(iq * bq, bq), bq)
    for w, out in ((wq, q_ref), (wk, k_ref)):
        t = _dot(a, _get(w)).astype(BF).astype(F32)
        for n, one in enumerate(jnp.split(t, heads, 1)):
            out[:, cols[n]] = (one * cos + pltpu.roll(one, HEAD // 2, 1) * sin).astype(BF)
    v = _dot(a, _get(wv)).astype(BF)
    v_ref[...] = v
    k_s[mine, :] = _get(k_ref)
    for c, one in zip(cut, jnp.split(v, heads, 1)):
        vt_s[c, mine] = jnp.concatenate([one.T, jnp.ones((8, bq), BF)], 0)
    top_s[...] = jnp.full_like(top_s, HUGE)
    mix_s[...] = jnp.zeros_like(mix_s)

    def block(at, size, pieces, ok):
        here, lane = pl.ds(at, size), pl.ds(pl.multiple_of(at, HEAD), size)
        scores = [_dot_t(k_s[here, cols[n]], q_ref[a:a+w, cols[n]]) for n, a, w in pieces]
        ps, keeps = [], []
        for (n, a, w), s in zip(pieces, scores):
            if ok is not None:
                s = jnp.where(ok, s, HUGE + HUGE)
            old = top_s[n:n+1, a:a+w]
            new = jnp.maximum(old, s.max(axis=0, keepdims=True))
            top_s[n:n+1, a:a+w] = new
            ps.append(jnp.exp2((s - new) * e).astype(BF))
            keeps.append(jnp.exp2((old - new) * e))
        for (n, a, w), p, keep in zip(pieces, ps, keeps):
            mix_s[cut[n], a:a+w] = mix_s[cut[n], a:a+w] * keep + _dot(vt_s[cut[n], lane], p)
    _loop(iq, lambda j: block(j * bq, bq, [(n, 0, bq) for n in range(heads)], None))
    seen = lambda w: lax.broadcasted_iota(jnp.int32, (half, w), 1) >= lax.broadcasted_iota(jnp.int32, (half, w), 0)
    block(iq * bq, half, [(n, 0, bq) for n in range(heads)], seen(bq))
    block(iq * bq + half, half, [(n, half, half) for n in range(heads)], seen(half))
    for n, (c, rows) in enumerate(zip(cols, cut)):
        mix = mix_s[rows, :]
        total = mix[HEAD:HEAD+1, :]
        o_ref[:, c] = (mix[:HEAD, :] * (1 / total)).T.astype(BF)
        lse_ref[n:n+1, :] = top_s[n:n+1, :] * e + jnp.log2(total)

def forward(h, wq, wk, wv, layer, before=(), bq=512):
    t, d = h.shape
    w = wq.shape[2]
    heads, second = w // HEAD, len(before) > 0
    rows = lambda n: pl.BlockSpec((bq, n), lambda i: (i, 0))
    tables = [jnp.asarray(a) for a in turns(t, bq)]
    state = lambda n: jax.ShapeDtypeStruct((t, n), BF)
    return pl.pallas_call(functools.partial(_forward, heads=heads, bq=bq, scale=HEAD**-0.5, second=second), grid=(t // bq,),
        in_specs=[rows(w)] * second + [_weight(m, layer - 1) for m in before[1:]] + [rows(d)] + [_weight(m, layer) for m in (wq, wk, wv)]
                 + [pl.BlockSpec(a.shape, lambda i: (0, 0), pipeline_mode=pl.Buffered(1)) for a in tables],
        out_specs=[rows(d)] * second + [rows(w)] * 4 + [pl.BlockSpec((heads, bq), lambda i: (0, i))],
        out_shape=[state(d)] * second + [state(w)] * 4 + [jax.ShapeDtypeStruct((heads, t), F32)],
        scratch_shapes=[pltpu.VMEM((heads * (HEAD + 8), t), BF), pltpu.VMEM((heads, bq), F32), pltpu.VMEM((heads * (HEAD + 8), bq), F32), pltpu.VMEM((t, w), BF)],
        compiler_params=_params("arbitrary"),
        cost_estimate=pl.CostEstimate(flops=2*t*t*w, bytes_accessed=12*t*w, transcendentals=heads*t*t//2), name="forward")(*before, h, wq, wk, wv, *tables)

MESH = pl.DeviceIdType.MESH

class Ring:
    def __init__(self, side):
        self.side, self.me = side, lax.axis_index("dp")
        at = self.me // side, self.me % side
        self.places = [[lax.rem(place + k, side) for k in range(side)] for place in at]

    def place(self, axis, away=0):
        return self.places[axis][away % self.side]

    def next(self, axis, sign):
        x, y = (self.place(n, sign if n == axis else 0) for n in range(2))
        return x * self.side + y

    def peers(self, far):
        many = self.side**2
        return [lax.rem(self.me + k, many) for k in range(1, many)] if far else [self.next(c // 2, _sign(c)) for c in range(4)]


def _sign(c):
    return 1 - c % 2 * 2


def _four(what, many=4):
    for c in range(many):
        what(c)


def _send(src, dst, send, recv, to):
    return pltpu.make_async_remote_copy(src_ref=src, dst_ref=dst, send_sem=send, recv_sem=recv, device_id={"dp": to}, device_id_type=MESH)


def _rows(ref, at, size):
    return ref.at[:, pl.ds(pl.multiple_of(at, size), size), :]


class Scatter:
    steps = 4

    def __init__(self, ring, own, buffers, send, recv, result):
        self.ring, self.own, self.send, self.recv, self.result = ring, own, send, recv, result
        self.xa, self.xb, self.ya_out, self.ya, self.yb_out, self.yb = buffers
        self.big, self.small = self.xb.shape[-2], self.yb.shape[-2]

    def mine(self, c, part, rows, size):
        return _rows(self.own.at[c // 2], self.ring.place(c // 2, part) * self.big + rows, size)

    def copies(self, c, s):
        sign, axis = _sign(c), (c // 2 + s // 2) % 2
        half = self.big // 2
        rows, other = c % 2 * half, (1 - c % 2) * half
        if s == 0:
            pairs = [(self.mine(c, 2, rows, half), self.xa.at[c])]
        elif s == 1:
            pairs = [(self.xa.at[c], _rows(self.xb.at[c], rows, half)), (self.mine(c, sign, other, half), _rows(self.xb.at[c], other, half))]
        else:
            pairs = [(self.ya_out.at[c], self.ya.at[c]) if s == 2 else (self.yb_out.at[c], self.yb.at[c])]
        return [_send(a, b, self.send, self.recv.at[s], self.ring.next(axis, sign)) for a, b in pairs]

    def total(self, half, part, rows, size):
        at = self.ring.place(1 - half, part) * self.small + rows
        got = [_get(_rows(self.xb.at[2 * half + n], at, size)).astype(F32) for n in range(2)]
        return got[0] + got[1] + _get(self.mine(2 * half, 0, at, size)).astype(F32)

    def ready(self, c, s):
        sign, half = _sign(c), self.small // 2
        rows = c % 2 * half
        if s == 1:
            self.xa[c] = (self.xa[c].astype(F32) + _get(self.mine(c, sign, c % 2 * (self.big // 2), self.big // 2)).astype(F32)).astype(BF)
        elif s == 2:
            self.ya_out[c] = self.total(c // 2, 2, rows, half).astype(BF)
        elif s == 3:
            _rows(self.yb_out.at[c], half - rows, half)[...] = self.total(c // 2, sign, half - rows, half).astype(BF)
            _rows(self.yb_out.at[c], rows, half)[...] = (self.total(c // 2, sign, rows, half) + self.ya[c].astype(F32)).astype(BF)

    def sent(self):
        same = self.own.at[:, :, pl.ds(0, 3 * (self.big + self.small)), :]
        _send(same, same, self.send, self.recv.at[0], self.ring.me).wait_send()

    def step(self, s):
        if s:
            got = (self.xa, self.xb, self.ya, self.yb)[s - 1]
            _send(got, got, self.send, self.recv.at[s - 1], self.ring.me).wait_recv()
        if s == self.steps:
            def close(half):
                total = self.total(half, 0, 0, self.small)
                self.result(half)[...] = (total + self.yb[2 * half].astype(F32) + self.yb[2 * half + 1].astype(F32)).astype(BF)
            _four(close, 2)
            return
        if s:
            _four(lambda c: self.ready(c, s))
        _four(lambda c: [one.start() for one in self.copies(c, s)])


class Gather:
    steps = 4

    def __init__(self, ring, whole, send, recv, base):
        self.ring, self.whole, self.send, self.recv, self.base = ring, whole, send, recv, base
        self.big = whole.shape[-2] // ring.side

    def place(self, half):
        small = self.big // self.ring.side
        return _rows(self.whole.at[half], self.ring.place(half) * self.big + self.ring.place(1 - half) * small, small)

    def copies(self, c, s):
        ring, sign, half = self.ring, _sign(c), c // 2
        axis = (1 - half) if s < 2 else half
        size = self.big // ring.side if s < 2 else self.big
        far = s % 2
        at = ring.place(axis, -sign * far) * size + far * (c % 2) * (size // 2)
        if s < 2:
            at = ring.place(half) * self.big + at
        part = _rows(self.whole.at[half], at, size // (1 + far))
        return _send(part, part, self.send, self.recv.at[self.base + s], ring.next(axis, sign))

    def step(self, s):
        if s:
            self.same((self.big if s > 2 else self.big // self.ring.side) * (1 + s % 2), s - 1).wait_recv()
        if s < self.steps:
            _four(lambda c: self.copies(c, s).start())

    def same(self, rows, s):
        part = self.whole.at[:, :, pl.ds(0, rows), :]
        return _send(part, part, self.send, self.recv.at[self.base + s], self.ring.me)

    def sent(self):
        self.same(3 * (self.big + self.big // self.ring.side), 0).wait_send()


class Job:
    def __init__(self, kind, matrices, time=1.0, made=False):
        self.kind, self.matrices, self.time, self.made, self.first, self.many = kind, matrices, time, made, 0, matrices
        self.sums, self.shares = kind != "share", kind != "sum"

    def sizes(self):
        return [self.matrices * BIG * k for k in ([0.5, 1, 0.125, 0.25] * self.sums + [0.25, 0.125, 1, 0.5] * self.shares)]


BIG, LAG = 1.43, 2.5


def plan(jobs, times):
    wire, state, out = 0.0, [(0, job.time) for job in jobs], []
    now = 0.0
    def advance():
        nonlocal wire
        picks = []
        for j, job in enumerate(jobs):
            s, ready = state[j]
            sizes = job.sizes()
            if s <= len(sizes) and ready <= now:
                picks.append((j, s))
                if s < len(sizes):
                    wire = max(wire, now) + sizes[s]
                state[j] = (s + 1, wire + LAG)
        return picks
    for now in times:
        out.append(advance())
    rest = []
    while todo := [ready for (s, ready), job in zip(state, jobs) if s <= len(job.sizes())]:
        now = max(now, min(todo))
        rest += advance()
    return out + [rest]


class Traffic:
    def __init__(self, jobs, side, rows, times, far=False):
        self.jobs, self.side, self.rows, self.far = jobs, side, rows, far
        self.plan = plan(jobs, times)
        small = rows // side**2
        hbm, vmem = pl.BlockSpec(memory_space=pltpu.HBM), lambda *s: pl.BlockSpec(s, lambda *_: (0,) * len(s), pipeline_mode=pl.Buffered(1))
        self.in_specs, self.out_specs, self.out_shape, self.scratch = [], [], [], []
        for job in jobs:
            unit = lambda many, size: (many, job.matrices, size, rows // 2)
            if not job.made:
                self.in_specs.append(hbm if job.sums else vmem(*unit(2, small)))
            if job is not jobs[0] and job.made and not job.shares:
                job.first = jobs[0].many
                jobs[0].many += job.matrices
            else:
                self.out_specs.append(hbm if job.shares else vmem)
                self.out_shape.append((job, rows if job.shares else small))
            if job.sums:
                sizes = (rows // side // 2, rows // side, small // 2, small // 2, small, small)
                self.scratch += [pltpu.VMEM(unit(2, rows), BF)] * (not job.made) + [pltpu.VMEM(unit(4, size), BF) for size in sizes]
            if job.shares:
                self.scratch.append(pltpu.VMEM(unit(2, rows), BF))
            self.scratch += [pltpu.SemaphoreType.DMA((2,)), pltpu.SemaphoreType.DMA((len(job.sizes()),)), pltpu.SemaphoreType.DMA((2,))]
        self.out_shape = [jax.ShapeDtypeStruct((2, job.many, size, rows // 2), BF) for job, size in self.out_shape] + [jax.ShapeDtypeStruct((8, HEAD), F32)]
        self.out_specs = [spec if spec is hbm else vmem(*a.shape) for spec, a in zip(self.out_specs + [vmem], self.out_shape)]

    def bind(self, ins, outs, scratch, made=()):
        ins, outs, scratch, made = iter(ins), iter(outs), iter(scratch), iter(made)
        self.ring = Ring(self.side)
        self.peers = self.ring.peers(self.far)
        self.run, self.mine = [], []
        for job in self.jobs:
            r = argparse.Namespace(given=None if job.made else next(ins), out=self.run[0].out if job.first else next(outs))
            if job.sums:
                r.own = next(made) if job.made else next(scratch)
                buffers = [next(scratch) for _ in range(6)]
            if job.shares:
                r.whole = next(scratch)
            send, recv, sem = (next(scratch) for _ in range(3))
            if job.shares:
                r.gather = Gather(self.ring, r.whole, send.at[1], recv, Scatter.steps * job.sums)
                r.store = pltpu.make_async_copy(r.whole, r.out, sem.at[1])
            if job.sums:
                r.scatter = Scatter(self.ring, r.own, buffers, send.at[0], recv, r.gather.place if job.shares else lambda half, r=r, job=job: r.out.at[half, pl.ds(job.first, job.matrices)])
                r.load = None if job.made else pltpu.make_async_copy(r.given, r.own, sem.at[0])
            self.run.append(r)
        self.squares = next(outs)

    def start(self):
        for job, r in zip(self.jobs, self.run):
            if job.sums and not job.made:
                r.load.start()
        self.squares[...] = jnp.zeros_like(self.squares)
        for peer in self.peers:
            pl.semaphore_signal(pltpu.get_barrier_semaphore(), inc=1, device_id={"dp": peer}, device_id_type=MESH)

    def meet(self):
        pl.semaphore_wait(pltpu.get_barrier_semaphore(), len(self.peers))

    def take(self, j, s):
        job, r = self.jobs[j], self.run[j]
        steps = Scatter.steps
        if s == 0 and not job.made and job.sums:
            r.load.wait()
        if job.sums and s <= steps:
            r.scatter.step(s)
            if s == steps:
                def fold(c):
                    got = r.scatter.result(c)[...].astype(F32)
                    got = (got * got).reshape(-1, 8, got.shape[-1]).sum(0)
                    self.squares[...] += sum(got[:, n:n + HEAD] for n in range(0, got.shape[-1], HEAD))
                _four(fold, 2)
        if job.shares and s >= steps * job.sums:
            if not job.sums and s == 0:
                def put(c):
                    r.gather.place(c)[...] = r.given[c]
                _four(put, 2)
            r.gather.step(s - steps * job.sums)
            if s == steps * (1 + job.sums):
                r.store.start()

    def tick(self, now, possible):
        for n in possible:
            picks = self.plan[n]
            if picks:
                @pl.when(now == n)
                def _():
                    for j, s in picks:
                        self.take(j, s)

    def finish(self):
        for j, s in self.plan[-1]:
            self.take(j, s)
        for job, r in zip(self.jobs, self.run):
            for part in ([r.scatter] if job.sums else []) + ([r.gather] if job.shares else []):
                part.sent()
            if job.shares:
                r.store.wait()


def _once(*shape):
    return pl.BlockSpec(shape, lambda *_: (0,) * len(shape), pipeline_mode=pl.Buffered(1))

def _comm(ident):
    return pltpu.CompilerParams(dimension_semantics=("arbitrary",), vmem_limit_bytes=MOST, collective_id=ident, has_side_effects=True)

MOST = 63 * 2**20

def _norm_back(x, s, by):
    by = by.astype(BF).astype(F32)
    return (s * by - x * (s * s * s * jnp.mean(by * x, -1, keepdims=True))).astype(BF).astype(F32)


def _split(to, value):
    for half, part in enumerate(jnp.split(value, 2, 1)):
        to(half)[...] = part.astype(BF)

def _half(*refs, block, sub, traffic, n_in, n_out, early):
    main, ins, rest, mine, outs, own, scratch = _cut(refs, 7, n_in, 1, 3, n_out, 16)
    *whole, wo, wg, wu, wd = main
    do_ref, delta_ref, dh_ref = mine
    h1_s, b_s, bt_s, dyt_s, act_s, dg_s, du_s, db_s, own_s, own_sem, o_ref, h_ref, dy_ref, do_s, sem, out_sem = own
    dh_s = h_ref
    c, last = pl.program_id(0), own_s.shape[0] - 1
    t, d = h_ref.shape
    per = t // block
    units = [own_s.at[n, :, pl.ds(0, 3)] for n in range(last)] + [own_s.at[last]]
    traffic.bind(ins, outs, scratch, units[:early])
    keep = [pltpu.make_async_copy(unit, rest[0].at[:, pl.ds(3 * n, unit.shape[1])], own_sem.at[n]) for n, unit in enumerate(units[early:])]
    at = lambda i: pl.ds(pl.multiple_of(i * block, block), block)
    loads = lambda i: [pltpu.make_async_copy(a.at[at(i), :], b.at[at(i), :], sem.at[n, i]) for n, (a, b) in enumerate(zip(whole, (o_ref, h_ref, dy_ref)))]
    stores = lambda i: [pltpu.make_async_copy(a.at[at(i), :], b.at[at(i), :], out_sem.at[n, i]) for n, (a, b) in enumerate(((do_s, do_ref), (dh_s, dh_ref)))]

    @pl.when(c == 0)
    def _():
        _loop(per, lambda i: _each(loads(i), "start"))
        traffic.start()
        def head(i):
            _each(loads(i), "wait")
            h1 = (h_ref[at(i), :].astype(F32) + _dot(o_ref[at(i), :], _get(wo)).astype(BF).astype(F32)).astype(BF)
            h1_s[at(i), :] = h1
            x, scale = _rms(h1)
            b = (x * scale).astype(BF)
            b_s[at(i), :] = b
            bt_s[:, at(i)] = b.T
            dyt_s[:, at(i)] = dy_ref[at(i), :].T
            db_s[at(i), :] = jnp.zeros((block, d), F32)
        _loop(per, head)
        traffic.meet()

    def body(i):
        traffic.tick(c * (per + 3) + i, [n for n in range((last + 1) * (per + 3)) if n % (per + 3) < per])
        rows = [pl.ds(i * block + k, sub) for k in range(0, block, sub)]
        first = [(_dot(b_s[r, :], _get(wg)), _dot(b_s[r, :], _get(wu)), _dot_t(dy_ref[r, :], _get(wd))) for r in rows]
        for r, (gate, up, dact) in zip(rows, first):
            dact = dact.astype(BF).astype(F32)
            sig = lax.logistic(gate)
            silu = gate * sig
            act_s[r, :] = (silu * up).astype(BF)
            du = (dact * silu).astype(BF)
            dg = (dact * up * (sig + silu * (1 - sig))).astype(BF)
            du_s[r, :] = du
            dg_s[r, :] = dg
            db_s[r, :] += _dot_t(dg, _get(wg)) + _dot_t(du, _get(wu))
    _loop(per, body)
    for m, value in enumerate((lambda: _dot(_get(bt_s), _get(dg_s)), lambda: _dot(_get(bt_s), _get(du_s)), lambda: _dot(_get(dyt_s), _get(act_s)).T)):
        traffic.tick(c * (per + 3) + per + m, range(per + m, (last + 1) * (per + 3), per + 3))
        _split(lambda k: own_s.at[c, k, m], value())
    for n, one in enumerate(keep[:-1]):
        pl.when(c == early + n)(one.start)

    @pl.when(c == last)
    def _():
        def tail(i):
            traffic.tick((last + 1) * (per + 3) + i, range((last + 1) * (per + 3), len(traffic.plan) - 1))
            x, s = _rms(h1_s[at(i), :])
            dh = (dy_ref[at(i), :].astype(F32) + _norm_back(x, s, db_s[at(i), :])).astype(BF)
            dh_s[at(i), :] = dh
            do = _dot_t(dh, _get(wo)).astype(BF)
            do_s[at(i), :] = do
            _each(stores(i), "start")
            prod = do.astype(F32) * o_ref[at(i), :].astype(F32)
            lane = lax.broadcasted_iota(jnp.int32, (block, HEAD), 1)
            sums = jnp.zeros((block, HEAD), F32)
            for n in range(prod.shape[1] // HEAD):
                sums = jnp.where(lane == n, prod[:, n*HEAD:(n+1)*HEAD].sum(-1, keepdims=True), sums)
            delta_ref[:, at(i)] = sums.T[:delta_ref.shape[0], :]
        _loop(per, tail)
        _split(lambda k: own_s.at[last, k, 3], _dot(_get(o_ref), _get(dh_s), 0, 0))
        keep[-1].start()
        traffic.finish()
        _each(keep, "wait")
        _loop(per, lambda i: _each(stores(i), "wait"))

def half_back(o, h, dy, wo, wg, wu, wd, layer, early, jobs, given, side, ident, block=512, sub=256, start=5.5, pace=1.75, dots=1.15, slow=1.3):
    t, d = h.shape
    e, f = o.shape[1], wg.shape[2]
    chunks, per = f // d, t // block
    times = []
    for c in range(chunks):
        now = start + c * (pace * per + dots * 3)
        times += [now + pace * i for i in range(per)] + [now + pace * per + dots * i for i in range(3)]
    times += [start + chunks * (pace * per + dots * 3) + slow * i for i in range(per)]
    made = [Job("sum", 3, start + (c + 1) * (pace * per + dots * 3), True) for c in range(early)]
    rest = jax.ShapeDtypeStruct((2, 3 * (chunks - early) + 1, d, d // 2), BF)
    traffic = Traffic(made + jobs, side, d, times)
    col, row = pl.BlockSpec((None, d, d), lambda c: (layer, 0, c)), pl.BlockSpec((None, d, d), lambda c: (layer, c, 0))
    big, hbm = lambda kind: pltpu.VMEM((t, d), kind), pl.BlockSpec(memory_space=pltpu.HBM)
    return pl.pallas_call(functools.partial(_half, block=block, sub=sub, traffic=traffic, n_in=len(given), n_out=len(traffic.out_specs), early=early), grid=(chunks,),
        in_specs=[hbm] * 3 + [_weight(wo, layer), col, col, row, *traffic.in_specs],
        out_specs=[hbm, hbm, _once(e // HEAD, t), hbm, *traffic.out_specs],
        out_shape=[rest, jax.ShapeDtypeStruct((t, e), BF), jax.ShapeDtypeStruct((e // HEAD, t), F32),
                   jax.ShapeDtypeStruct((t, d), BF), *traffic.out_shape],
        scratch_shapes=[big(BF), big(BF), pltpu.VMEM((d, t), BF), pltpu.VMEM((d, t), BF), big(BF), big(BF), big(BF), big(F32),
                        pltpu.VMEM((chunks, 2, 4, d, d // 2), BF), pltpu.SemaphoreType.DMA((chunks,)), *[big(BF)] * 4, *[pltpu.SemaphoreType.DMA((3, per))] * 2, *traffic.scratch],
        compiler_params=_comm(ident),
        cost_estimate=pl.CostEstimate(flops=2*t*(3*d*e+8*d*f), bytes_accessed=12*t*d, transcendentals=0),
        name="half_back")(o, h, dy, wo, wg, wu, wd, *given)

def _clip(traffic, known, count, factor_ref, sums_s, one_s, send, recv):
    me, n = traffic.ring.me, traffic.side**2
    copy = lambda peer, slot: _send(one_s, sums_s.at[slot], send.at[lax.rem(peer - me + n, n)], recv.at[slot], peer)
    left = [j for j, s in traffic.plan[-1] if traffic.jobs[j].sums and s == Scatter.steps]
    for j, s in traffic.plan[-1]:
        traffic.take(j, s)
        if left and j == left[-1] and s == Scatter.steps:
            one_s[...] = sum((_get(ref) for ref in known), _get(traffic.squares))
            sums_s[me] = _get(one_s)
            for peer in traffic.peers:
                copy(peer, me).start()
    traffic.plan[-1].clear()
    for peer in traffic.peers:
        copy(peer, peer).wait_recv()
    total = functools.reduce(jnp.add, [sums_s[k] for k in range(n)])
    factor_ref[...] = jnp.broadcast_to(jnp.minimum(1.0, 0.5 * lax.rsqrt(jnp.sum(total, keepdims=True) / count + 1e-30)), factor_ref.shape)
    for peer in traffic.peers:
        copy(peer, me).wait_send()

def _first(*refs, heads, bq, scale, deep, layer, traffic, n_in, n_out, known, count):
    last_one = not deep
    main, late, ins, known, unit, dx_ref, factor_ref, outs, own, held, clip, scratch = _cut(refs, 11, 4 * deep, n_in, known, deep, deep, last_one, n_out, 10, 6 * deep, 5 * last_one)
    q_ref, k_new, v_new, do_ref, lse_ref, delta_ref, h_ref, cl, sl, ch, sh = main
    kt_s, dq_s, dk_s, dv_s, q_s, at_s, k_s, v_s, k_ref, v_ref = own
    loads = []
    if deep:
        h_s, dh_s, wq, wk, wv, sem = held
        loads = [pltpu.make_async_copy(a if n == 0 else a.at[layer], b, sem.at[n]) for n, (a, b) in enumerate(zip(late, held[1:]))]
    iq, last = pl.program_id(0), k_ref.shape[0] // bq - 1
    e = scale * LOG2E
    half = bq // 2
    cols = [pl.ds(n * HEAD, HEAD) for n in range(heads)]
    at = lambda i: pl.ds(pl.multiple_of(i * bq, bq), bq)
    mine = at(iq)
    *clip, unit_ref = clip + unit
    traffic.bind(ins, outs, scratch, [unit_ref.at[:, pl.ds(m, 1)] for m in range(unit_ref.shape[1])])

    @pl.when(iq == 0)
    def _():
        traffic.start()
        _each(loads, "start")
    x, s = _rms(_get(h_ref))
    at_s[:, mine] = (x * s).astype(BF).T
    if deep:
        h_s[mine, :] = _get(h_ref)
    k_ref[mine, :] = _get(k_new)
    v_ref[mine, :] = _get(v_new)
    for c in cols:
        kt_s[c, mine] = k_new[:, c].T
    dq_s[...] = jnp.zeros_like(dq_s)
    dk_s[mine, :] = jnp.zeros((bq, k_ref.shape[1]), F32)
    dv_s[mine, :] = jnp.zeros((bq, k_ref.shape[1]), F32)

    def block(at, size, pieces, ok):
        here, lane = pl.ds(at, size), pl.ds(pl.multiple_of(at, HEAD), size)
        scores = [_dot_t(k_ref[here, cols[n]], q_ref[a:a+w, cols[n]]) for n, a, w in pieces]
        dps = [_dot_t(v_ref[here, cols[n]], do_ref[a:a+w, cols[n]]) for n, a, w in pieces]
        for (n, a, w), s, dp in zip(pieces, scores, dps):
            p = jnp.exp2(s * e - lse_ref[n:n+1, a:a+w])
            if ok is not None:
                p = jnp.where(ok, p, 0.0)
            ds = (p * (dp - delta_ref[n:n+1, a:a+w])).astype(BF)
            dv_s[here, cols[n]] += _dot(p.astype(BF), do_ref[a:a+w, cols[n]])
            dk_s[here, cols[n]] += _dot(ds, q_ref[a:a+w, cols[n]])
            dq_s[cols[n], a:a+w] += _dot(kt_s[cols[n], lane], ds)

    pl.when(iq == 0)(traffic.meet)
    before = iq * (iq + 1) // 2
    cuts = list(itertools.accumulate(range(1, last + 2), initial=0))
    *cuts, ticks = [n for n in cuts[:-1]] + [cuts[-1]]
    cuts = [n + k for k, n in enumerate(cuts)]
    def off(j):
        traffic.tick(before + j, [n for n in range(ticks) if n not in cuts])
        block(j * bq, bq, [(n, 0, bq) for n in range(heads)], None)
    _loop(iq, off)
    traffic.tick(before + iq, cuts)
    seen = lambda w: lax.broadcasted_iota(jnp.int32, (half, w), 1) >= lax.broadcasted_iota(jnp.int32, (half, w), 0)
    block(iq * bq, half, [(n, 0, bq) for n in range(heads)], seen(bq))
    block(iq * bq + half, half, [(n, half, half) for n in range(heads)], seen(half))

    def unturned(i, value):
        c, s = _angles(i, cl, sl, ch, sh)
        one = (value * scale).astype(BF).astype(F32)
        return (one * c - pltpu.roll(one, HEAD // 2, 1) * s).astype(BF)
    for c in cols:
        q_s[mine, c] = unturned(iq, dq_s[c, :].T)

    @pl.when(iq == last)
    def _():
        _each(loads, "wait")
        def tail(i):
            traffic.tick(ticks + i, range(ticks, ticks + last + 1))
            for c in cols:
                k_s[at(i), c] = unturned(i, dk_s[at(i), c])
            v_s[at(i), :] = dv_s[at(i), :].astype(BF)
            if deep:
                by = _dot_t(q_s[at(i), :], _get(wq)) + _dot_t(k_s[at(i), :], _get(wk)) + _dot_t(v_s[at(i), :], _get(wv))
                x, s = _rms(h_s[at(i), :])
                dx_ref[0][at(i), :] = (dh_s[at(i), :].astype(F32) + _norm_back(x, s, by)).astype(BF)
        _loop(last + 1, tail)
        for m, value in enumerate((q_s, k_s, v_s)):
            traffic.tick(ticks + last + 1 + m, [ticks + last + 1 + m])
            _split(lambda k: unit_ref.at[k, m], _dot(_get(at_s), _get(value)))
        if last_one:
            _clip(traffic, known, count, *factor_ref, *clip)
        traffic.finish()


def first_back(q, k, v, do, lse, delta, h, dh, wq, wk, wv, layer, deep, jobs, given, known, count, side, ident, bq=512, start=2.0, pace=3.5, more=3.2, end=1.3):
    t, w = q.shape
    d, heads = h.shape[1], w // HEAD
    now, times = start, []
    for i in range(t // bq):
        times += [now + pace * j for j in range(i + 1)]
        now += pace * i + more
    times += [now + end * i for i in range(t // bq + 3)]
    jobs = jobs + [Job("both", 1, time + end, True) for time in times[-3:]] * (not deep)
    traffic = Traffic(jobs, side, d, times, not deep)
    rows, stats = pl.BlockSpec((bq, w), lambda i: (i, 0)), pl.BlockSpec((heads, bq), lambda i: (0, i))
    tables = [jnp.asarray(a) for a in turns(t, bq)]
    big = lambda kind: pltpu.VMEM((t, w), kind)
    late, n = [dh, wq, wk, wv] * deep, side**2
    unit, tile = (2, 3, d, d // 2), jax.ShapeDtypeStruct((8, HEAD), F32)
    results = [jax.ShapeDtypeStruct(unit, BF), jax.ShapeDtypeStruct((t, d), BF)] if deep else [tile]
    clip = [pltpu.VMEM((n, *tile.shape), F32), pltpu.VMEM(tile.shape, F32), *[pltpu.SemaphoreType.DMA((n,))] * 2, pltpu.VMEM(unit, BF)] * (not deep)
    held = [pltpu.VMEM((t, d), BF)] * 2 * deep + [pltpu.VMEM(m.shape[1:], BF) for m in late[1:]] + [pltpu.SemaphoreType.DMA((len(late),))] * deep
    return pl.pallas_call(functools.partial(_first, heads=heads, bq=bq, scale=HEAD**-0.5, deep=deep, layer=layer, traffic=traffic, n_in=len(given),
                          n_out=len(traffic.out_specs), known=len(known), count=count),
        grid=(t // bq,),
        in_specs=[rows] * 4 + [stats, stats, pl.BlockSpec((bq, d), lambda i: (i, 0)), *(_once(*a.shape) for a in tables),
                  *[pl.BlockSpec(memory_space=pltpu.HBM)] * len(late), *traffic.in_specs, *[_once(*tile.shape)] * len(known)],
        out_specs=[_once(*a.shape) for a in results] + traffic.out_specs, out_shape=results + traffic.out_shape,
        scratch_shapes=[pltpu.VMEM((w, t), BF), pltpu.VMEM((w, bq), F32), big(F32), big(F32), big(BF), pltpu.VMEM((d, t), BF), *[big(BF)] * 4, *held, *clip, *traffic.scratch],
        compiler_params=_comm(ident),
        cost_estimate=pl.CostEstimate(flops=5*t*t*w, bytes_accessed=14*t*w, transcendentals=heads*t*t//2),
        name="first_back")(q, k, v, do, lse, delta, h, *tables, *late, *given, *known)

def _adam(*refs, arrays, units, places, slots, ahead, piece):
    (factor_ref,), w, m, v, g, new, (w_s, m_s, v_s, g_s, load, store) = _cut(refs, 1, *[arrays] * 3, units, 3 * arrays)
    factor = factor_ref[:1, :1]
    d = w_s.shape[2]

    def loads(i):
        array, layer, row, col, unit, matrix, part = places[i]
        k = i % slots
        spot = lambda a: a.at[layer, pl.ds(row, piece), pl.ds(col, d)]
        pairs = [(spot(a[array]), b.at[k]) for a, b in ((w, w_s), (m, m_s), (v, v_s))] + [(g[unit].at[:, matrix, pl.ds(part, piece), :], g_s.at[k])]
        return [pltpu.make_async_copy(a, b, load.at[k, n]) for n, (a, b) in enumerate(pairs)]

    def stores(i):
        array, layer, row, col, *_ = places[i]
        k = i % slots
        return [pltpu.make_async_copy(a.at[k], new[n * arrays + array].at[layer, pl.ds(row, piece), pl.ds(col, d)], store.at[k, n])
                for n, a in enumerate((w_s, m_s, v_s))]

    for i in range(min(ahead, len(places))):
        _each(loads(i), "start")
    for i in range(len(places)):
        _each(loads(i), "wait")
        k = i % slots
        def update(r):
            rows = pl.ds(r * 32, 32)
            for c in range(2):
                cols = pl.ds(c * (d // 2), d // 2)
                grad = g_s[k, c, rows, :].astype(F32) * factor
                first = 0.9 * m_s[k, rows, cols] + 0.1 * grad
                second = 0.95 * v_s[k, rows, cols] + 0.05 * grad * grad
                old = w_s[k, rows, cols].astype(F32)
                m_s[k, rows, cols] = first
                v_s[k, rows, cols] = second
                w_s[k, rows, cols] = (old - 0.02 * (first * lax.rsqrt(second + 1e-8) + 0.1 * old)).astype(BF)
        _loop(piece // 32, update)
        _each(stores(i), "start")
        if i + ahead < len(places):
            if i + ahead >= slots:
                _each(stores(i + ahead - slots), "wait")
            _each(loads(i + ahead), "start")
    for i in range(max(len(places) - slots, 0), len(places)):
        _each(stores(i), "wait")

def adam(factor, w, m, v, units, slots=12, ahead=6, piece=512):
    d = w[0].shape[1]
    places, flat = [], []
    for layer, mine in reversed(list(enumerate(units))):
        spots = [(unit, matrix) for unit, a in enumerate(mine) for matrix in range(a.shape[1])]
        arrays = [(array, 0, n * d) if array < 6 else (array, n * d, 0) for n in range(w[4].shape[2] // d) for array in (4, 5, 6)] + [(i, 0, 0) for i in (3, 0, 1, 2)]
        places += [(array, layer, row + part, col, len(flat) + unit, matrix, part) for (array, row, col), (unit, matrix) in zip(arrays, spots) for part in range(0, d, piece)]
        flat += mine
    hbm = pl.BlockSpec(memory_space=pltpu.HBM)
    size = sum(a.size for a in w)
    return pl.pallas_call(functools.partial(_adam, arrays=len(w), units=len(flat), places=places, slots=slots, ahead=ahead, piece=piece), grid=(1,),
        in_specs=[_once(8, HEAD)] + [hbm] * (3 * len(w) + len(flat)), out_specs=[hbm] * (3 * len(w)),
        out_shape=[jax.ShapeDtypeStruct(a.shape, a.dtype) for a in (*w, *m, *v)],
        scratch_shapes=[pltpu.VMEM((slots, piece, d), BF), pltpu.VMEM((slots, piece, d), F32), pltpu.VMEM((slots, piece, d), F32), pltpu.VMEM((slots, 2, piece, d // 2), BF),
                        pltpu.SemaphoreType.DMA((slots, 4)), pltpu.SemaphoreType.DMA((slots, 3))],
        compiler_params=pltpu.CompilerParams(dimension_semantics=("arbitrary",), vmem_limit_bytes=VMEM),
        cost_estimate=pl.CostEstimate(flops=16*size, bytes_accessed=22*size, transcendentals=size), name="adam")(factor, *w, *m, *v, *flat)


def solution(mesh):
    side = round(mesh.shape["dp"] ** 0.5)

    def step(x, dy, *arrays):
        weights, m, v = (arrays[i : i + 7] for i in (0, 7, 14))
        wq, wk, wv, wo, wg, wu, wd = weights
        h0 = x[0]
        q0, k0, v0, o0, lse0 = forward(h0, wq, wk, wv, 0)
        h1, q1, k1, v1, o1, lse1 = forward(h0, wq, wk, wv, 1, (o0, wo, wg, wu, wd))
        add, share = (lambda n, kind=kind: Job(kind, n) for kind in ("sum", "share"))
        late1, do1, delta1, by1, s10, sq0 = half_back(o1, h1, dy[0], wo, wg, wu, wd, 1, 3, [], [], side, 0)
        attn1, by0, s11, g10, sq1 = first_back(q1, k1, v1, do1, lse1, delta1, h1, by1, wq, wk, wv, 1, True, [add(4), share(9)], [late1, s10], [], None, side, 1)
        late0, do0, delta0, by, s00, g12, g11, sq2 = half_back(o0, h0, by0, wo, wg, wu, wd, 0, 3, [Job("both", 3), share(4)], [attn1, s11], side, 2)
        factor, g01, g00, *g02, _ = first_back(q0, k0, v0, do0, lse0, delta0, h0, by, wq, wk, wv, 0, False, [Job("both", 4), share(9)], [late0, s00],
                                               [sq0, sq1, sq2], sum(w.size for w in weights), side, 3)
        return adam(factor, weights, m, v, [[g00, g01, *g02], [g10, g11, g12]])

    states, all_of = P(("rep", "dp"), None, None), P(None, None, None)
    return jax.shard_map(step, mesh=mesh, in_specs=(states, states) + (all_of,) * 21, out_specs=(P("rep", None, None),) * 21, check_vma=False)
```

```python
import argparse
import functools
import itertools

import jax
import jax.numpy as jnp
import numpy as np
from jax import lax
from jax.experimental import pallas as pl
from jax.experimental.pallas import tpu as pltpu
from jax.sharding import PartitionSpec as P

HEAD=128; THETA=10000
BF=jnp.bfloat16; F32=jnp.float32
VMEM = 56 * 2**20
LOG2E = 1.4426950408889634
HUGE = -1e30

def _dot(a, b, ca=1, cb=0):
    return lax.dot_general(a, b, (((ca,), (cb,)), ((), ())), preferred_element_type=F32)

def _dot_t(a, b):
    return _dot(a, b, 1, 1)

def _get(ref):
    return ref[...]

def _loop(many, what):
    lax.fori_loop(0, many, lambda i, _: what(i), None)

def _each(copies, what):
    for one in copies:
        getattr(one, what)()

def _cut(refs, *sizes):
    refs = iter(refs)
    return [list(itertools.islice(refs, size)) for size in sizes] + [list(refs)]

def _params(*sem, limit=VMEM):
    return pltpu.CompilerParams(dimension_semantics=sem, vmem_limit_bytes=limit)

def turns(tokens, block):
    half = HEAD // 2
    speed = THETA ** (-np.arange(half) / half)
    def pair(places):
        angle = places[:, None] * speed
        return (np.concatenate([np.cos(angle)] * 2, 1).astype(np.float32), np.concatenate([np.sin(angle)] * 2, 1).astype(np.float32))
    return (*pair(np.arange(block)), *pair(np.arange(0, tokens, block)))

def _rms(h):
    wide = h.astype(F32)
    return wide, lax.rsqrt(jnp.mean(wide * wide, -1, keepdims=True) + 1e-6)

def _angles(i, cl, sl, ch, sh):
    c0, s0 = ch[pl.ds(i, 1), :], sh[pl.ds(i, 1), :]
    c = _get(cl) * c0 - _get(sl) * s0
    s = _get(sl) * c0 + _get(cl) * s0
    lane = lax.broadcasted_iota(jnp.int32, s.shape, 1)
    return c, jnp.where(lane < HEAD // 2, -s, s)

def _weight(w, layer):
    return pl.BlockSpec((None, *w.shape[1:]), lambda *_: (layer, 0, 0), pipeline_mode=pl.Buffered(1))

def _forward(*refs, heads, bq, scale, second):
    before, (h_ref, wq, wk, wv, cl, sl, ch, sh), h1_ref, outs, own = _cut(refs, 5 * second, 8, second, 5)
    q_ref, k_ref, v_ref, o_ref, lse_ref = outs
    vt_s, top_s, mix_s, k_s = own
    iq = pl.program_id(0)
    e = scale * LOG2E
    half = bq // 2
    h = _get(h_ref)
    if second:
        last_ref, wo, wg, wu, wd = before
        h = (h.astype(F32) + _dot(_get(last_ref), _get(wo)).astype(BF).astype(F32)).astype(BF)
        x, s = _rms(h)
        b = (x * s).astype(BF)
        total = []
        for c in range(0, wg.shape[1], bq):
            gate = _dot(b, wg[:, c:c+bq])
            act = (gate * lax.logistic(gate) * _dot(b, wu[:, c:c+bq])).astype(BF)
            total.append(_dot(act, wd[c:c+bq, :]))
        h = (h.astype(F32) + functools.reduce(jnp.add, total).astype(BF).astype(F32)).astype(BF)
        h1_ref[0][...] = h
    x, s = _rms(h)
    a = (x * s).astype(BF)
    cos, sin = _angles(iq, cl, sl, ch, sh)
    cols = [pl.ds(n * HEAD, HEAD) for n in range(heads)]
    cut = [pl.ds(n * (HEAD + 8), HEAD + 8) for n in range(heads)]
    mine = pl.ds(pl.multiple_of(iq * bq, bq), bq)
    for w, out in ((wq, q_ref), (wk, k_ref)):
        t = _dot(a, _get(w)).astype(BF).astype(F32)
        for n, one in enumerate(jnp.split(t, heads, 1)):
            out[:, cols[n]] = (one * cos + pltpu.roll(one, HEAD // 2, 1) * sin).astype(BF)
    v = _dot(a, _get(wv)).astype(BF)
    v_ref[...] = v
    k_s[mine, :] = _get(k_ref)
    for c, one in zip(cut, jnp.split(v, heads, 1)):
        vt_s[c, mine] = jnp.concatenate([one.T, jnp.ones((8, bq), BF)], 0)
    top_s[...] = jnp.full_like(top_s, HUGE)
    mix_s[...] = jnp.zeros_like(mix_s)

    def block(at, size, pieces, ok):
        here, lane = pl.ds(at, size), pl.ds(pl.multiple_of(at, HEAD), size)
        scores = [_dot_t(k_s[here, cols[n]], q_ref[a:a+w, cols[n]]) for n, a, w in pieces]
        ps, keeps = [], []
        for (n, a, w), s in zip(pieces, scores):
            if ok is not None:
                s = jnp.where(ok, s, HUGE + HUGE)
            old = top_s[n:n+1, a:a+w]
            new = jnp.maximum(old, s.max(axis=0, keepdims=True))
            top_s[n:n+1, a:a+w] = new
            ps.append(jnp.exp2((s - new) * e).astype(BF))
            keeps.append(jnp.exp2((old - new) * e))
        for (n, a, w), p, keep in zip(pieces, ps, keeps):
            mix_s[cut[n], a:a+w] = mix_s[cut[n], a:a+w] * keep + _dot(vt_s[cut[n], lane], p)
    _loop(iq, lambda j: block(j * bq, bq, [(n, 0, bq) for n in range(heads)], None))
    seen = lambda w: lax.broadcasted_iota(jnp.int32, (half, w), 1) >= lax.broadcasted_iota(jnp.int32, (half, w), 0)
    block(iq * bq, half, [(n, 0, bq) for n in range(heads)], seen(bq))
    block(iq * bq + half, half, [(n, half, half) for n in range(heads)], seen(half))
    for n, (c, rows) in enumerate(zip(cols, cut)):
        mix = mix_s[rows, :]
        total = mix[HEAD:HEAD+1, :]
        o_ref[:, c] = (mix[:HEAD, :] * (1 / total)).T.astype(BF)
        lse_ref[n:n+1, :] = top_s[n:n+1, :] * e + jnp.log2(total)

def forward(h, wq, wk, wv, layer, before=(), bq=512):
    t, d = h.shape
    w = wq.shape[2]
    heads, second = w // HEAD, len(before) > 0
    rows = lambda n: pl.BlockSpec((bq, n), lambda i: (i, 0))
    tables = [jnp.asarray(a) for a in turns(t, bq)]
    state = lambda n: jax.ShapeDtypeStruct((t, n), BF)
    return pl.pallas_call(functools.partial(_forward, heads=heads, bq=bq, scale=HEAD**-0.5, second=second), grid=(t // bq,),
        in_specs=[rows(w)] * second + [_weight(m, layer - 1) for m in before[1:]] + [rows(d)] + [_weight(m, layer) for m in (wq, wk, wv)]
                 + [pl.BlockSpec(a.shape, lambda i: (0, 0), pipeline_mode=pl.Buffered(1)) for a in tables],
        out_specs=[rows(d)] * second + [rows(w)] * 4 + [pl.BlockSpec((heads, bq), lambda i: (0, i))],
        out_shape=[state(d)] * second + [state(w)] * 4 + [jax.ShapeDtypeStruct((heads, t), F32)],
        scratch_shapes=[pltpu.VMEM((heads * (HEAD + 8), t), BF), pltpu.VMEM((heads, bq), F32), pltpu.VMEM((heads * (HEAD + 8), bq), F32), pltpu.VMEM((t, w), BF)],
        compiler_params=_params("arbitrary"),
        cost_estimate=pl.CostEstimate(flops=2*t*t*w, bytes_accessed=12*t*w, transcendentals=heads*t*t//2), name="forward")(*before, h, wq, wk, wv, *tables)

MESH = pl.DeviceIdType.MESH

class Ring:
    def __init__(self, side):
        self.side, self.me = side, lax.axis_index("dp")
        at = self.me // side, self.me % side
        self.places = [[lax.rem(place + k, side) for k in range(side)] for place in at]

    def place(self, axis, away=0):
        return self.places[axis][away % self.side]

    def next(self, axis, sign):
        x, y = (self.place(n, sign if n == axis else 0) for n in range(2))
        return x * self.side + y

    def peers(self, far):
        many = self.side**2
        return [lax.rem(self.me + k, many) for k in range(1, many)] if far else [self.next(c // 2, _sign(c)) for c in range(4)]


def _sign(c):
    return 1 - c % 2 * 2


def _four(what, many=4):
    for c in range(many):
        what(c)


def _send(src, dst, send, recv, to):
    return pltpu.make_async_remote_copy(src_ref=src, dst_ref=dst, send_sem=send, recv_sem=recv, device_id={"dp": to}, device_id_type=MESH)


def _rows(ref, at, size):
    return ref.at[:, pl.ds(pl.multiple_of(at, size), size), :]


class Scatter:
    steps = 4

    def __init__(self, ring, own, buffers, send, recv, result):
        self.ring, self.own, self.send, self.recv, self.result = ring, own, send, recv, result
        self.xa, self.xb, self.ya_out, self.ya, self.yb_out, self.yb = buffers
        self.big, self.small = self.xb.shape[-2], self.yb.shape[-2]

    def mine(self, c, part, rows, size):
        return _rows(self.own.at[c // 2], self.ring.place(c // 2, part) * self.big + rows, size)

    def copies(self, c, s):
        sign, axis = _sign(c), (c // 2 + s // 2) % 2
        half = self.big // 2
        rows, other = c % 2 * half, (1 - c % 2) * half
        if s == 0:
            pairs = [(self.mine(c, 2, rows, half), self.xa.at[c])]
        elif s == 1:
            pairs = [(self.xa.at[c], _rows(self.xb.at[c], rows, half)), (self.mine(c, sign, other, half), _rows(self.xb.at[c], other, half))]
        else:
            pairs = [(self.ya_out.at[c], self.ya.at[c]) if s == 2 else (self.yb_out.at[c], self.yb.at[c])]
        return [_send(a, b, self.send, self.recv.at[s], self.ring.next(axis, sign)) for a, b in pairs]

    def total(self, half, part, rows, size):
        at = self.ring.place(1 - half, part) * self.small + rows
        got = [_get(_rows(self.xb.at[2 * half + n], at, size)).astype(F32) for n in range(2)]
        return got[0] + got[1] + _get(self.mine(2 * half, 0, at, size)).astype(F32)

    def ready(self, c, s):
        sign, half = _sign(c), self.small // 2
        rows = c % 2 * half
        if s == 1:
            self.xa[c] = (self.xa[c].astype(F32) + _get(self.mine(c, sign, c % 2 * (self.big // 2), self.big // 2)).astype(F32)).astype(BF)
        elif s == 2:
            self.ya_out[c] = self.total(c // 2, 2, rows, half).astype(BF)
        elif s == 3:
            _rows(self.yb_out.at[c], half - rows, half)[...] = self.total(c // 2, sign, half - rows, half).astype(BF)
            _rows(self.yb_out.at[c], rows, half)[...] = (self.total(c // 2, sign, rows, half) + self.ya[c].astype(F32)).astype(BF)

    def sent(self):
        same = self.own.at[:, :, pl.ds(0, 3 * (self.big + self.small)), :]
        _send(same, same, self.send, self.recv.at[0], self.ring.me).wait_send()

    def step(self, s):
        if s:
            got = (self.xa, self.xb, self.ya, self.yb)[s - 1]
            _send(got, got, self.send, self.recv.at[s - 1], self.ring.me).wait_recv()
        if s == self.steps:
            def close(half):
                total = self.total(half, 0, 0, self.small)
                self.result(half)[...] = (total + self.yb[2 * half].astype(F32) + self.yb[2 * half + 1].astype(F32)).astype(BF)
            _four(close, 2)
            return
        if s:
            _four(lambda c: self.ready(c, s))
        _four(lambda c: [one.start() for one in self.copies(c, s)])


class Gather:
    steps = 4

    def __init__(self, ring, whole, send, recv, base):
        self.ring, self.whole, self.send, self.recv, self.base = ring, whole, send, recv, base
        self.big = whole.shape[-2] // ring.side

    def place(self, half):
        small = self.big // self.ring.side
        return _rows(self.whole.at[half], self.ring.place(half) * self.big + self.ring.place(1 - half) * small, small)

    def copies(self, c, s):
        ring, sign, half = self.ring, _sign(c), c // 2
        axis = (1 - half) if s < 2 else half
        size = self.big // ring.side if s < 2 else self.big
        far = s % 2
        at = ring.place(axis, -sign * far) * size + far * (c % 2) * (size // 2)
        if s < 2:
            at = ring.place(half) * self.big + at
        part = _rows(self.whole.at[half], at, size // (1 + far))
        return _send(part, part, self.send, self.recv.at[self.base + s], ring.next(axis, sign))

    def step(self, s):
        if s:
            self.same((self.big if s > 2 else self.big // self.ring.side) * (1 + s % 2), s - 1).wait_recv()
        if s < self.steps:
            _four(lambda c: self.copies(c, s).start())

    def same(self, rows, s):
        part = self.whole.at[:, :, pl.ds(0, rows), :]
        return _send(part, part, self.send, self.recv.at[self.base + s], self.ring.me)

    def sent(self):
        self.same(3 * (self.big + self.big // self.ring.side), 0).wait_send()


class Job:
    def __init__(self, kind, matrices, time=1.0, made=False):
        self.kind, self.matrices, self.time, self.made, self.first, self.many = kind, matrices, time, made, 0, matrices
        self.sums, self.shares = kind != "share", kind != "sum"

    def sizes(self):
        return [self.matrices * BIG * k for k in ([0.5, 1, 0.125, 0.25] * self.sums + [0.25, 0.125, 1, 0.5] * self.shares)]


BIG, LAG = 1.43, 1.8


def plan(jobs, times):
    wire, state, out = 0.0, [(0, job.time) for job in jobs], []
    now = 0.0
    def advance():
        nonlocal wire
        picks = []
        for j, job in enumerate(jobs):
            s, ready = state[j]
            sizes = job.sizes()
            if s <= len(sizes) and ready <= now:
                picks.append((j, s))
                if s < len(sizes):
                    wire = max(wire, now) + sizes[s]
                state[j] = (s + 1, wire + LAG)
        return picks
    for now in times:
        out.append(advance())
    rest = []
    while todo := [ready for (s, ready), job in zip(state, jobs) if s <= len(job.sizes())]:
        now = max(now, min(todo))
        rest += advance()
    return out + [rest]


class Traffic:
    def __init__(self, jobs, side, rows, times, far=False):
        self.jobs, self.side, self.rows, self.far = jobs, side, rows, far
        self.plan = plan(jobs, times)
        small = rows // side**2
        hbm, vmem = pl.BlockSpec(memory_space=pltpu.HBM), lambda *s: pl.BlockSpec(s, lambda *_: (0,) * len(s), pipeline_mode=pl.Buffered(1))
        self.in_specs, self.out_specs, self.out_shape, self.scratch = [], [], [], []
        for job in jobs:
            unit = lambda many, size: (many, job.matrices, size, rows // 2)
            if not job.made:
                self.in_specs.append(hbm if job.sums else vmem(*unit(2, small)))
            if job is not jobs[0] and job.made and not job.shares:
                job.first = jobs[0].many
                jobs[0].many += job.matrices
            else:
                self.out_specs.append(hbm if job.shares else vmem)
                self.out_shape.append((job, rows if job.shares else small))
            if job.sums:
                sizes = (rows // side // 2, rows // side, small // 2, small // 2, small, small)
                self.scratch += [pltpu.VMEM(unit(2, rows), BF)] * (not job.made) + [pltpu.VMEM(unit(4, size), BF) for size in sizes]
            if job.shares:
                self.scratch.append(pltpu.VMEM(unit(2, rows), BF))
            self.scratch += [pltpu.SemaphoreType.DMA((2,)), pltpu.SemaphoreType.DMA((len(job.sizes()),)), pltpu.SemaphoreType.DMA((2,))]
        self.out_shape = [jax.ShapeDtypeStruct((2, job.many, size, rows // 2), BF) for job, size in self.out_shape] + [jax.ShapeDtypeStruct((8, HEAD), F32)]
        self.out_specs = [spec if spec is hbm else vmem(*a.shape) for spec, a in zip(self.out_specs + [vmem], self.out_shape)]

    def bind(self, ins, outs, scratch, made=()):
        ins, outs, scratch, made = iter(ins), iter(outs), iter(scratch), iter(made)
        self.ring = Ring(self.side)
        self.peers = self.ring.peers(self.far)
        self.run, self.mine = [], []
        for job in self.jobs:
            r = argparse.Namespace(given=None if job.made else next(ins), out=self.run[0].out if job.first else next(outs))
            if job.sums:
                r.own = next(made) if job.made else next(scratch)
                buffers = [next(scratch) for _ in range(6)]
            if job.shares:
                r.whole = next(scratch)
            send, recv, sem = (next(scratch) for _ in range(3))
            if job.shares:
                r.gather = Gather(self.ring, r.whole, send.at[1], recv, Scatter.steps * job.sums)
                r.store = pltpu.make_async_copy(r.whole, r.out, sem.at[1])
            if job.sums:
                r.scatter = Scatter(self.ring, r.own, buffers, send.at[0], recv, r.gather.place if job.shares else lambda half, r=r, job=job: r.out.at[half, pl.ds(job.first, job.matrices)])
                r.load = None if job.made else pltpu.make_async_copy(r.given, r.own, sem.at[0])
            self.run.append(r)
        self.squares = next(outs)

    def start(self):
        for job, r in zip(self.jobs, self.run):
            if job.sums and not job.made:
                r.load.start()
        self.squares[...] = jnp.zeros_like(self.squares)
        for peer in self.peers:
            pl.semaphore_signal(pltpu.get_barrier_semaphore(), inc=1, device_id={"dp": peer}, device_id_type=MESH)

    def meet(self):
        pl.semaphore_wait(pltpu.get_barrier_semaphore(), len(self.peers))

    def take(self, j, s):
        job, r = self.jobs[j], self.run[j]
        steps = Scatter.steps
        if s == 0 and not job.made and job.sums:
            r.load.wait()
        if job.sums and s <= steps:
            r.scatter.step(s)
            if s == steps:
                def fold(c):
                    got = r.scatter.result(c)[...].astype(F32)
                    got = (got * got).reshape(-1, 8, got.shape[-1]).sum(0)
                    self.squares[...] += sum(got[:, n:n + HEAD] for n in range(0, got.shape[-1], HEAD))
                _four(fold, 2)
        if job.shares and s >= steps * job.sums:
            if not job.sums and s == 0:
                def put(c):
                    r.gather.place(c)[...] = r.given[c]
                _four(put, 2)
            r.gather.step(s - steps * job.sums)
            if s == steps * (1 + job.sums):
                r.store.start()

    def tick(self, now, possible):
        for n in possible:
            picks = self.plan[n]
            if picks:
                @pl.when(now == n)
                def _():
                    for j, s in picks:
                        self.take(j, s)

    def finish(self):
        for j, s in self.plan[-1]:
            self.take(j, s)
        for job, r in zip(self.jobs, self.run):
            for part in ([r.scatter] if job.sums else []) + ([r.gather] if job.shares else []):
                part.sent()
            if job.shares:
                r.store.wait()


def _once(*shape):
    return pl.BlockSpec(shape, lambda *_: (0,) * len(shape), pipeline_mode=pl.Buffered(1))

def _comm(ident):
    return pltpu.CompilerParams(dimension_semantics=("arbitrary",), vmem_limit_bytes=MOST, collective_id=ident, has_side_effects=True)

MOST = 63 * 2**20

def _norm_back(x, s, by):
    by = by.astype(BF).astype(F32)
    return (s * by - x * (s * s * s * jnp.mean(by * x, -1, keepdims=True))).astype(BF).astype(F32)


def _split(to, value):
    for half, part in enumerate(jnp.split(value, 2, 1)):
        to(half)[...] = part.astype(BF)

def _half(*refs, block, sub, traffic, n_in, n_out, early):
    main, ins, rest, mine, outs, own, scratch = _cut(refs, 7, n_in, 1, 3, n_out, 16)
    *whole, wo, wg, wu, wd = main
    do_ref, delta_ref, dh_ref = mine
    h1_s, b_s, bt_s, dyt_s, act_s, dg_s, du_s, db_s, own_s, own_sem, o_ref, h_ref, dy_ref, do_s, sem, out_sem = own
    dh_s = h_ref
    c, last = pl.program_id(0), own_s.shape[0] - 1
    t, d = h_ref.shape
    per = t // block
    units = [own_s.at[n, :, pl.ds(0, 3)] for n in range(last)] + [own_s.at[last]]
    traffic.bind(ins, outs, scratch, units[:early])
    keep = [pltpu.make_async_copy(unit, rest[0].at[:, pl.ds(3 * n, unit.shape[1])], own_sem.at[n]) for n, unit in enumerate(units[early:])]
    at = lambda i: pl.ds(pl.multiple_of(i * block, block), block)
    loads = lambda i: [pltpu.make_async_copy(a.at[at(i), :], b.at[at(i), :], sem.at[n, i]) for n, (a, b) in enumerate(zip(whole, (o_ref, h_ref, dy_ref)))]
    stores = lambda i: [pltpu.make_async_copy(a.at[at(i), :], b.at[at(i), :], out_sem.at[n, i]) for n, (a, b) in enumerate(((do_s, do_ref), (dh_s, dh_ref)))]

    @pl.when(c == 0)
    def _():
        _loop(per, lambda i: _each(loads(i), "start"))
        traffic.start()
        def head(i):
            _each(loads(i), "wait")
            h1 = (h_ref[at(i), :].astype(F32) + _dot(o_ref[at(i), :], _get(wo)).astype(BF).astype(F32)).astype(BF)
            h1_s[at(i), :] = h1
            x, scale = _rms(h1)
            b = (x * scale).astype(BF)
            b_s[at(i), :] = b
            bt_s[:, at(i)] = b.T
            dyt_s[:, at(i)] = dy_ref[at(i), :].T
            db_s[at(i), :] = jnp.zeros((block, d), F32)
        _loop(per, head)
        traffic.meet()

    def body(i):
        traffic.tick(c * (per + 3) + i, [n for n in range((last + 1) * (per + 3)) if n % (per + 3) < per])
        rows = [pl.ds(i * block + k, sub) for k in range(0, block, sub)]
        first = [(_dot(b_s[r, :], _get(wg)), _dot(b_s[r, :], _get(wu)), _dot_t(dy_ref[r, :], _get(wd))) for r in rows]
        for r, (gate, up, dact) in zip(rows, first):
            dact = dact.astype(BF).astype(F32)
            sig = lax.logistic(gate)
            silu = gate * sig
            act_s[r, :] = (silu * up).astype(BF)
            du = (dact * silu).astype(BF)
            dg = (dact * up * (sig + silu * (1 - sig))).astype(BF)
            du_s[r, :] = du
            dg_s[r, :] = dg
            db_s[r, :] += _dot_t(dg, _get(wg)) + _dot_t(du, _get(wu))
    _loop(per, body)
    for m, value in enumerate((lambda: _dot(_get(bt_s), _get(dg_s)), lambda: _dot(_get(bt_s), _get(du_s)), lambda: _dot(_get(dyt_s), _get(act_s)).T)):
        traffic.tick(c * (per + 3) + per + m, range(per + m, (last + 1) * (per + 3), per + 3))
        _split(lambda k: own_s.at[c, k, m], value())
    for n, one in enumerate(keep[:-1]):
        pl.when(c == early + n)(one.start)

    @pl.when(c == last)
    def _():
        def tail(i):
            traffic.tick((last + 1) * (per + 3) + i, range((last + 1) * (per + 3), len(traffic.plan) - 1))
            x, s = _rms(h1_s[at(i), :])
            dh = (dy_ref[at(i), :].astype(F32) + _norm_back(x, s, db_s[at(i), :])).astype(BF)
            dh_s[at(i), :] = dh
            do = _dot_t(dh, _get(wo)).astype(BF)
            do_s[at(i), :] = do
            _each(stores(i), "start")
            prod = do.astype(F32) * o_ref[at(i), :].astype(F32)
            lane = lax.broadcasted_iota(jnp.int32, (block, HEAD), 1)
            sums = jnp.zeros((block, HEAD), F32)
            for n in range(prod.shape[1] // HEAD):
                sums = jnp.where(lane == n, prod[:, n*HEAD:(n+1)*HEAD].sum(-1, keepdims=True), sums)
            delta_ref[:, at(i)] = sums.T[:delta_ref.shape[0], :]
        _loop(per, tail)
        _split(lambda k: own_s.at[last, k, 3], _dot(_get(o_ref), _get(dh_s), 0, 0))
        keep[-1].start()
        traffic.finish()
        _each(keep, "wait")
        _loop(per, lambda i: _each(stores(i), "wait"))

def half_back(o, h, dy, wo, wg, wu, wd, layer, early, jobs, given, side, ident, block=512, sub=256, start=5.5, pace=1.75, dots=1.15, slow=1.3):
    t, d = h.shape
    e, f = o.shape[1], wg.shape[2]
    chunks, per = f // d, t // block
    times = []
    for c in range(chunks):
        now = start + c * (pace * per + dots * 3)
        times += [now + pace * i for i in range(per)] + [now + pace * per + dots * i for i in range(3)]
    times += [start + chunks * (pace * per + dots * 3) + slow * i for i in range(per)]
    made = [Job("sum", 3, start + (c + 1) * (pace * per + dots * 3), True) for c in range(early)]
    rest = jax.ShapeDtypeStruct((2, 3 * (chunks - early) + 1, d, d // 2), BF)
    traffic = Traffic(made + jobs, side, d, times)
    col, row = pl.BlockSpec((None, d, d), lambda c: (layer, 0, c)), pl.BlockSpec((None, d, d), lambda c: (layer, c, 0))
    big, hbm = lambda kind: pltpu.VMEM((t, d), kind), pl.BlockSpec(memory_space=pltpu.HBM)
    return pl.pallas_call(functools.partial(_half, block=block, sub=sub, traffic=traffic, n_in=len(given), n_out=len(traffic.out_specs), early=early), grid=(chunks,),
        in_specs=[hbm] * 3 + [_weight(wo, layer), col, col, row, *traffic.in_specs],
        out_specs=[hbm, hbm, _once(e // HEAD, t), hbm, *traffic.out_specs],
        out_shape=[rest, jax.ShapeDtypeStruct((t, e), BF), jax.ShapeDtypeStruct((e // HEAD, t), F32),
                   jax.ShapeDtypeStruct((t, d), BF), *traffic.out_shape],
        scratch_shapes=[big(BF), big(BF), pltpu.VMEM((d, t), BF), pltpu.VMEM((d, t), BF), big(BF), big(BF), big(BF), big(F32),
                        pltpu.VMEM((chunks, 2, 4, d, d // 2), BF), pltpu.SemaphoreType.DMA((chunks,)), *[big(BF)] * 4, *[pltpu.SemaphoreType.DMA((3, per))] * 2, *traffic.scratch],
        compiler_params=_comm(ident),
        cost_estimate=pl.CostEstimate(flops=2*t*(3*d*e+8*d*f), bytes_accessed=12*t*d, transcendentals=0),
        name="half_back")(o, h, dy, wo, wg, wu, wd, *given)

def _clip(traffic, known, count, factor_ref, sums_s, one_s, send, recv):
    me, n = traffic.ring.me, traffic.side**2
    copy = lambda peer, slot: _send(one_s, sums_s.at[slot], send.at[lax.rem(peer - me + n, n)], recv.at[slot], peer)
    left = [j for j, s in traffic.plan[-1] if traffic.jobs[j].sums and s == Scatter.steps]
    for j, s in traffic.plan[-1]:
        traffic.take(j, s)
        if left and j == left[-1] and s == Scatter.steps:
            one_s[...] = sum((_get(ref) for ref in known), _get(traffic.squares))
            sums_s[me] = _get(one_s)
            for peer in traffic.peers:
                copy(peer, me).start()
    traffic.plan[-1].clear()
    for peer in traffic.peers:
        copy(peer, peer).wait_recv()
    total = functools.reduce(jnp.add, [sums_s[k] for k in range(n)])
    factor_ref[...] = jnp.broadcast_to(jnp.minimum(1.0, 0.5 * lax.rsqrt(jnp.sum(total, keepdims=True) / count + 1e-30)), factor_ref.shape)
    for peer in traffic.peers:
        copy(peer, me).wait_send()

def _first(*refs, heads, bq, scale, deep, layer, traffic, n_in, n_out, known, count):
    last_one = not deep
    main, late, ins, known, unit, dx_ref, factor_ref, outs, own, held, clip, scratch = _cut(refs, 11, 4 * deep, n_in, known, deep, deep, last_one, n_out, 10, 6 * deep, 5 * last_one)
    q_ref, k_new, v_new, do_ref, lse_ref, delta_ref, h_ref, cl, sl, ch, sh = main
    kt_s, dq_s, dk_s, dv_s, q_s, at_s, k_s, v_s, k_ref, v_ref = own
    loads = []
    if deep:
        h_s, dh_s, wq, wk, wv, sem = held
        loads = [pltpu.make_async_copy(a if n == 0 else a.at[layer], b, sem.at[n]) for n, (a, b) in enumerate(zip(late, held[1:]))]
    iq, last = pl.program_id(0), k_ref.shape[0] // bq - 1
    e = scale * LOG2E
    half = bq // 2
    cols = [pl.ds(n * HEAD, HEAD) for n in range(heads)]
    at = lambda i: pl.ds(pl.multiple_of(i * bq, bq), bq)
    mine = at(iq)
    *clip, unit_ref = clip + unit
    traffic.bind(ins, outs, scratch, [unit_ref.at[:, pl.ds(m, 1)] for m in range(unit_ref.shape[1])])

    @pl.when(iq == 0)
    def _():
        traffic.start()
        _each(loads, "start")
    x, s = _rms(_get(h_ref))
    at_s[:, mine] = (x * s).astype(BF).T
    if deep:
        h_s[mine, :] = _get(h_ref)
    k_ref[mine, :] = _get(k_new)
    v_ref[mine, :] = _get(v_new)
    for c in cols:
        kt_s[c, mine] = k_new[:, c].T
    dq_s[...] = jnp.zeros_like(dq_s)
    dk_s[mine, :] = jnp.zeros((bq, k_ref.shape[1]), F32)
    dv_s[mine, :] = jnp.zeros((bq, k_ref.shape[1]), F32)

    def block(at, size, pieces, ok):
        here, lane = pl.ds(at, size), pl.ds(pl.multiple_of(at, HEAD), size)
        scores = [_dot_t(k_ref[here, cols[n]], q_ref[a:a+w, cols[n]]) for n, a, w in pieces]
        dps = [_dot_t(v_ref[here, cols[n]], do_ref[a:a+w, cols[n]]) for n, a, w in pieces]
        for (n, a, w), s, dp in zip(pieces, scores, dps):
            p = jnp.exp2(s * e - lse_ref[n:n+1, a:a+w])
            if ok is not None:
                p = jnp.where(ok, p, 0.0)
            ds = (p * (dp - delta_ref[n:n+1, a:a+w])).astype(BF)
            dv_s[here, cols[n]] += _dot(p.astype(BF), do_ref[a:a+w, cols[n]])
            dk_s[here, cols[n]] += _dot(ds, q_ref[a:a+w, cols[n]])
            dq_s[cols[n], a:a+w] += _dot(kt_s[cols[n], lane], ds)

    pl.when(iq == 0)(traffic.meet)
    before = iq * (iq + 1) // 2
    cuts = list(itertools.accumulate(range(1, last + 2), initial=0))
    *cuts, ticks = [n for n in cuts[:-1]] + [cuts[-1]]
    cuts = [n + k for k, n in enumerate(cuts)]
    def off(j):
        traffic.tick(before + j, [n for n in range(ticks) if n not in cuts])
        block(j * bq, bq, [(n, 0, bq) for n in range(heads)], None)
    _loop(iq, off)
    traffic.tick(before + iq, cuts)
    seen = lambda w: lax.broadcasted_iota(jnp.int32, (half, w), 1) >= lax.broadcasted_iota(jnp.int32, (half, w), 0)
    block(iq * bq, half, [(n, 0, bq) for n in range(heads)], seen(bq))
    block(iq * bq + half, half, [(n, half, half) for n in range(heads)], seen(half))

    def unturned(i, value):
        c, s = _angles(i, cl, sl, ch, sh)
        one = (value * scale).astype(BF).astype(F32)
        return (one * c - pltpu.roll(one, HEAD // 2, 1) * s).astype(BF)
    for c in cols:
        q_s[mine, c] = unturned(iq, dq_s[c, :].T)

    @pl.when(iq == last)
    def _():
        _each(loads, "wait")
        def tail(i):
            traffic.tick(ticks + i, range(ticks, ticks + last + 1))
            for c in cols:
                k_s[at(i), c] = unturned(i, dk_s[at(i), c])
            v_s[at(i), :] = dv_s[at(i), :].astype(BF)
            if deep:
                by = _dot_t(q_s[at(i), :], _get(wq)) + _dot_t(k_s[at(i), :], _get(wk)) + _dot_t(v_s[at(i), :], _get(wv))
                x, s = _rms(h_s[at(i), :])
                dx_ref[0][at(i), :] = (dh_s[at(i), :].astype(F32) + _norm_back(x, s, by)).astype(BF)
        _loop(last + 1, tail)
        for m, value in enumerate((q_s, k_s, v_s)):
            traffic.tick(ticks + last + 1 + m, [ticks + last + 1 + m])
            _split(lambda k: unit_ref.at[k, m], _dot(_get(at_s), _get(value)))
        if last_one:
            _clip(traffic, known, count, *factor_ref, *clip)
        traffic.finish()


def first_back(q, k, v, do, lse, delta, h, dh, wq, wk, wv, layer, deep, jobs, given, known, count, side, ident, bq=512, start=2.0, pace=3.5, more=3.2, end=1.3):
    t, w = q.shape
    d, heads = h.shape[1], w // HEAD
    now, times = start, []
    for i in range(t // bq):
        times += [now + pace * j for j in range(i + 1)]
        now += pace * i + more
    times += [now + end * i for i in range(t // bq + 3)]
    jobs = jobs + [Job("both", 1, time + end, True) for time in times[-3:]] * (not deep)
    traffic = Traffic(jobs, side, d, times, not deep)
    rows, stats = pl.BlockSpec((bq, w), lambda i: (i, 0)), pl.BlockSpec((heads, bq), lambda i: (0, i))
    tables = [jnp.asarray(a) for a in turns(t, bq)]
    big = lambda kind: pltpu.VMEM((t, w), kind)
    late, n = [dh, wq, wk, wv] * deep, side**2
    unit, tile = (2, 3, d, d // 2), jax.ShapeDtypeStruct((8, HEAD), F32)
    results = [jax.ShapeDtypeStruct(unit, BF), jax.ShapeDtypeStruct((t, d), BF)] if deep else [tile]
    clip = [pltpu.VMEM((n, *tile.shape), F32), pltpu.VMEM(tile.shape, F32), *[pltpu.SemaphoreType.DMA((n,))] * 2, pltpu.VMEM(unit, BF)] * (not deep)
    held = [pltpu.VMEM((t, d), BF)] * 2 * deep + [pltpu.VMEM(m.shape[1:], BF) for m in late[1:]] + [pltpu.SemaphoreType.DMA((len(late),))] * deep
    return pl.pallas_call(functools.partial(_first, heads=heads, bq=bq, scale=HEAD**-0.5, deep=deep, layer=layer, traffic=traffic, n_in=len(given),
                          n_out=len(traffic.out_specs), known=len(known), count=count),
        grid=(t // bq,),
        in_specs=[rows] * 4 + [stats, stats, pl.BlockSpec((bq, d), lambda i: (i, 0)), *(_once(*a.shape) for a in tables),
                  *[pl.BlockSpec(memory_space=pltpu.HBM)] * len(late), *traffic.in_specs, *[_once(*tile.shape)] * len(known)],
        out_specs=[_once(*a.shape) for a in results] + traffic.out_specs, out_shape=results + traffic.out_shape,
        scratch_shapes=[pltpu.VMEM((w, t), BF), pltpu.VMEM((w, bq), F32), big(F32), big(F32), big(BF), pltpu.VMEM((d, t), BF), *[big(BF)] * 4, *held, *clip, *traffic.scratch],
        compiler_params=_comm(ident),
        cost_estimate=pl.CostEstimate(flops=5*t*t*w, bytes_accessed=14*t*w, transcendentals=heads*t*t//2),
        name="first_back")(q, k, v, do, lse, delta, h, *tables, *late, *given, *known)

def _adam(*refs, arrays, units, places, slots, ahead, piece):
    (factor_ref,), w, m, v, g, new, (w_s, m_s, v_s, g_s, load, store) = _cut(refs, 1, *[arrays] * 3, units, 3 * arrays)
    factor = factor_ref[:1, :1]
    d = w_s.shape[2]

    def loads(i):
        array, layer, row, col, unit, matrix, part = places[i]
        k = i % slots
        spot = lambda a: a.at[layer, pl.ds(row, piece), pl.ds(col, d)]
        pairs = [(spot(a[array]), b.at[k]) for a, b in ((w, w_s), (m, m_s), (v, v_s))] + [(g[unit].at[:, matrix, pl.ds(part, piece), :], g_s.at[k])]
        return [pltpu.make_async_copy(a, b, load.at[k, n]) for n, (a, b) in enumerate(pairs)]

    def stores(i):
        array, layer, row, col, *_ = places[i]
        k = i % slots
        return [pltpu.make_async_copy(a.at[k], new[n * arrays + array].at[layer, pl.ds(row, piece), pl.ds(col, d)], store.at[k, n])
                for n, a in enumerate((w_s, m_s, v_s))]

    for i in range(min(ahead, len(places))):
        _each(loads(i), "start")
    for i in range(len(places)):
        _each(loads(i), "wait")
        k = i % slots
        def update(r):
            rows = pl.ds(r * 32, 32)
            for c in range(2):
                cols = pl.ds(c * (d // 2), d // 2)
                grad = g_s[k, c, rows, :].astype(F32) * factor
                first = 0.9 * m_s[k, rows, cols] + 0.1 * grad
                second = 0.95 * v_s[k, rows, cols] + 0.05 * grad * grad
                old = w_s[k, rows, cols].astype(F32)
                m_s[k, rows, cols] = first
                v_s[k, rows, cols] = second
                w_s[k, rows, cols] = (old - 0.02 * (first * lax.rsqrt(second + 1e-8) + 0.1 * old)).astype(BF)
        _loop(piece // 32, update)
        _each(stores(i), "start")
        if i + ahead < len(places):
            if i + ahead >= slots:
                _each(stores(i + ahead - slots), "wait")
            _each(loads(i + ahead), "start")
    for i in range(max(len(places) - slots, 0), len(places)):
        _each(stores(i), "wait")

def adam(factor, w, m, v, units, slots=12, ahead=6, piece=512):
    d = w[0].shape[1]
    places, flat = [], []
    for layer, mine in reversed(list(enumerate(units))):
        spots = [(unit, matrix) for unit, a in enumerate(mine) for matrix in range(a.shape[1])]
        arrays = [(array, 0, n * d) if array < 6 else (array, n * d, 0) for n in range(w[4].shape[2] // d) for array in (4, 5, 6)] + [(i, 0, 0) for i in (3, 0, 1, 2)]
        places += [(array, layer, row + part, col, len(flat) + unit, matrix, part) for (array, row, col), (unit, matrix) in zip(arrays, spots) for part in range(0, d, piece)]
        flat += mine
    hbm = pl.BlockSpec(memory_space=pltpu.HBM)
    size = sum(a.size for a in w)
    return pl.pallas_call(functools.partial(_adam, arrays=len(w), units=len(flat), places=places, slots=slots, ahead=ahead, piece=piece), grid=(1,),
        in_specs=[_once(8, HEAD)] + [hbm] * (3 * len(w) + len(flat)), out_specs=[hbm] * (3 * len(w)),
        out_shape=[jax.ShapeDtypeStruct(a.shape, a.dtype) for a in (*w, *m, *v)],
        scratch_shapes=[pltpu.VMEM((slots, piece, d), BF), pltpu.VMEM((slots, piece, d), F32), pltpu.VMEM((slots, piece, d), F32), pltpu.VMEM((slots, 2, piece, d // 2), BF),
                        pltpu.SemaphoreType.DMA((slots, 4)), pltpu.SemaphoreType.DMA((slots, 3))],
        compiler_params=pltpu.CompilerParams(dimension_semantics=("arbitrary",), vmem_limit_bytes=VMEM),
        cost_estimate=pl.CostEstimate(flops=16*size, bytes_accessed=22*size, transcendentals=size), name="adam")(factor, *w, *m, *v, *flat)


def solution(mesh):
    side = round(mesh.shape["dp"] ** 0.5)

    def step(x, dy, *arrays):
        weights, m, v = (arrays[i : i + 7] for i in (0, 7, 14))
        wq, wk, wv, wo, wg, wu, wd = weights
        h0 = x[0]
        q0, k0, v0, o0, lse0 = forward(h0, wq, wk, wv, 0)
        h1, q1, k1, v1, o1, lse1 = forward(h0, wq, wk, wv, 1, (o0, wo, wg, wu, wd))
        add, share = (lambda n, kind=kind: Job(kind, n) for kind in ("sum", "share"))
        late1, do1, delta1, by1, s10, sq0 = half_back(o1, h1, dy[0], wo, wg, wu, wd, 1, 3, [], [], side, 0)
        attn1, by0, s11, g10, sq1 = first_back(q1, k1, v1, do1, lse1, delta1, h1, by1, wq, wk, wv, 1, True, [add(4), share(9)], [late1, s10], [], None, side, 1)
        late0, do0, delta0, by, s00, g12, g11, sq2 = half_back(o0, h0, by0, wo, wg, wu, wd, 0, 3, [Job("both", 3), share(4)], [attn1, s11], side, 2)
        factor, g01, g00, *g02, _ = first_back(q0, k0, v0, do0, lse0, delta0, h0, by, wq, wk, wv, 0, False, [Job("both", 4), share(9)], [late0, s00],
                                               [sq0, sq1, sq2], sum(w.size for w in weights), side, 3)
        return adam(factor, weights, m, v, [[g00, g01, *g02], [g10, g11, g12]])

    states, all_of = P(("rep", "dp"), None, None), P(None, None, None)
    return jax.shard_map(step, mesh=mesh, in_specs=(states, states) + (all_of,) * 21, out_specs=(P("rep", None, None),) * 21, check_vma=False)
```
